128 devices in a mesh: expert: 32 (over y, x, core), dp: 4 (over z).
Axes of the slice: x: 4, y: 4, z: 4, core: 2. Of those that a mesh axis runs over, the one named last changes fastest.
Arguments:
- out_grads: bfloat16 [4, 4096, 7168], P('dp', 'expert'), may hold values from -6 to 6
- expert_ids: int32 [4, 4096, 8], P('dp', 'expert'), may hold values from 0 to 255, all different within a row; in each aligned block of 128 rows (0 to 127, 128 to 255, ..., all dimensions but the last counted through in order) at most 6 rows name the same one
- gate_probs: float32 [4, 4096, 8], P('dp', 'expert'), may hold values from 0.05 to 0.5
- hidden_acts: bfloat16 [4, 256, 192, 2048], P('dp', 'expert'), may hold values from -6 to 6
- q_previous: bfloat16 [256, 32, 7168], P('expert'), may hold values from -0.0625 to 0.0625
Outputs:
- new_basis: float32 [256, 32, 2048], P('expert')
- q_update: float32 [256, 32, 7168], P('expert', None, 'dp')
The draws below stay inside these ranges and needn't reach their ends.
Inputs may be any that keep to these rules, and one draw needn't show every extreme that they name: `expert_ids`: each row names 8 different experts; among the rows of one device no expert is named more than 6 times.
All inputs are finite; a program needn't handle non-finite values.
Results may differ from the reference program's by a relative error of at most 0.014.
Values may be sent and summed in bfloat16 or wider, within the bound.
No kernel may reach another device: no remote copies, remote signals or barrier semaphores. Data moves between devices by JAX's collectives and lax.ppermute only.
A program may use at most 192 MiB of HBM per device.

```python
import math
import jax
import jax.numpy as jnp
import numpy as np
from jax import lax

D = 7168
FF = 2048
TOP = 8
RANK = 32
TOK_DEV = 128
EXPERTS = 256
CAP = 6
SLOTS = 192
TOK_EXP = 4096
N_EXPERT = 32
N_DP = 4


def steps_of(key, extent, shards, smallest, top_value):
    factor_of, own = 1.0, jax.random.fold_in(key, 6)
    for dim, parts in shards:
        heights = jnp.exp(jax.random.uniform(jax.random.fold_in(own, dim), (parts,), jnp.float32, smallest / len(shards), top_value / len(shards)))
        factor_of = factor_of * jnp.repeat(heights, extent[dim] // parts).reshape([-1 if axis == dim else 1 for axis in range(len(extent))])
    return factor_of


def routed_block(rng, own, number, rows, count, top, limit, skew):
    ranking = jax.random.permutation(rng, count)
    crowded, usual = portions_of(count, rows * top, limit, skew, True), portions_of(count, rows * top, limit, skew, False)
    places = jnp.arange(count)

    def named(tallies, rotation):
        used = int((tallies > 0).sum())
        fixed = max(1, used // 4)
        passed = fixed + (places - fixed + rotation * (used - fixed)) % max(1, count - fixed)
        return jnp.zeros((count,), jnp.int32).at[ranking[jnp.where(places < fixed, places, passed)]].set(jnp.asarray(tallies, jnp.int32))

    tallies = jnp.where(number % 4 == 0, named(crowded, number // 4), named(usual, number - number // 4 - 1))
    mixed = jax.random.permutation(jax.random.fold_in(own, 3), count)
    source_of, sink = mixed[0:count // 2 * 2:2], mixed[1:count // 2 * 2:2]
    room = jnp.minimum(tallies[source_of] - 1, limit - tallies[sink]) // 2
    room = jnp.where((source_of == ranking[0]) | (sink == ranking[0]) | (tallies[sink] == 0), 0, jnp.maximum(room, 0))
    passed = jax.random.randint(jax.random.fold_in(own, 4), (count // 2,), 0, 1 << 20) % (room + 1)
    tallies = tallies.at[source_of].add(-passed).at[sink].add(passed)
    labels = jnp.searchsorted(jnp.cumsum(tallies), jnp.arange(rows * top), side="right").astype(jnp.int32)
    grid = labels.reshape(top, rows).T
    grid = grid[jax.random.permutation(jax.random.fold_in(own, 1), rows)]
    rotation = jax.random.randint(jax.random.fold_in(own, 2), (rows, 1), 0, top)
    return jnp.take_along_axis(grid, (jnp.arange(top)[None, :] + rotation) % top, axis=1)


def portions_of(number_of, total, bound, slope, full):
    weights = [(1 << 20) // math.isqrt(grade ** slope) + 1 for grade in range(1, number_of + 1)]
    largest = bound if full else min(bound, max(-(-total // number_of), total * weights[0] // sum(weights)))
    least = 1 if total - largest >= number_of - 1 else 0
    given, surplus = [largest] + [least] * (number_of - 1), total - largest - least * (number_of - 1)
    while surplus > 0:
        free = [i for i in range(1, number_of) if given[i] < largest] or [i for i in range(1, number_of) if given[i] < bound]
        mass, budget = sum([weights[i] for i in free]), surplus
        for i in free:
            more = min(bound - given[i], max(1, budget * weights[i] // mass), surplus)
            given[i] = given[i] + more
            surplus = surplus - more
    return np.array(given)


def noise(key, shape, deviation, bound, cuts=(), kind=jnp.bfloat16):
    factor_of = steps_of(key, shape, cuts, -0.22, 0.18) if cuts else 1.0
    result = jax.random.normal(key, shape, jnp.float32) * deviation * factor_of
    return jnp.minimum(jnp.maximum(result, -bound), bound).astype(kind)


def setup_inputs(seed: int = 0) -> dict:
    arg_keys = jax.random.split(jax.random.key(seed), 6)
    out_grads = noise(arg_keys[0], (N_DP, TOK_EXP, D), 1.0, 6.0, ((0, 4), (1, 32)))
    expert_ids_keys = jax.random.split(jax.random.fold_in(arg_keys[1], 1), N_DP * TOK_EXP // TOK_DEV)
    expert_ids_turns = jax.random.permutation(jax.random.fold_in(arg_keys[1], 3), N_DP * TOK_EXP // TOK_DEV)
    expert_ids = jax.vmap(lambda own, number: routed_block(jax.random.fold_in(arg_keys[1], 2), own, number, TOK_DEV, EXPERTS, TOP, CAP, 1))(expert_ids_keys, expert_ids_turns).reshape((N_DP, TOK_EXP, TOP))
    gate_probs = jnp.clip(0.05 + 0.45 * jax.random.uniform(arg_keys[2], (N_DP, TOK_EXP, TOP), jnp.float32) ** steps_of(arg_keys[2], (N_DP, TOK_EXP, TOP), ((0, 4), (1, 32)), -0.2, 0.2), 0.05, 0.5)
    hidden_acts = noise(arg_keys[3], (N_DP, EXPERTS, SLOTS, FF), 1.0, 6.0, ((0, 4), (1, 32)))
    q_previous = noise(arg_keys[4], (EXPERTS, RANK, D), D ** -0.5, 0.0625, ((0, 32),))
    return {"out_grads": out_grads, "expert_ids": expert_ids, "gate_probs": gate_probs, "hidden_acts": hidden_acts, "q_previous": q_previous}


def to_half(values):
    return lax.optimization_barrier(values.astype(jnp.bfloat16))

def slot_tables(route_ids, gate_values, num_experts, capacity):
    flat_ids = route_ids.reshape(-1)
    row_count = flat_ids.shape[0]
    top_k = route_ids.shape[-1]
    one_hot = (flat_ids[:, None] == jnp.arange(num_experts, dtype=jnp.int32)[None, :]).astype(jnp.int32)
    earlier = jnp.cumsum(one_hot, axis=0) - one_hot
    position = lax.optimization_barrier(jnp.sum(earlier * one_hot, axis=1)).astype(jnp.int32)
    slot_index = (flat_ids * capacity + position).astype(jnp.int32)
    token_of = jnp.zeros((num_experts * capacity,), jnp.int32).at[slot_index].set((jnp.arange(row_count, dtype=jnp.int32) // top_k).astype(jnp.int32))
    gate_of = jnp.zeros((num_experts * capacity,), jnp.float32).at[slot_index].set(gate_values.reshape(-1).astype(jnp.float32))
    return (token_of, gate_of)

def reference(out_grads, expert_ids, gate_probs, hidden_acts, q_previous):
    grads_blocks = out_grads.reshape(N_DP, N_EXPERT, TOK_DEV, D)
    id_blocks = expert_ids.reshape(N_DP, N_EXPERT, TOK_DEV, TOP)
    gate_blocks = gate_probs.reshape(N_DP, N_EXPERT, TOK_DEV, TOP)
    tables = jax.vmap(jax.vmap(lambda ids, gts: slot_tables(ids, gts, EXPERTS, CAP)))
    token_of, gate_of = tables(id_blocks, gate_blocks)

    def pick_rows(grads_one, tokens_one):
        return jnp.take(grads_one, tokens_one, axis=0)

    def one_expert(expert_num):
        start = (expert_num * CAP).astype(jnp.int32)
        tokens_here = lax.dynamic_slice_in_dim(token_of, start, CAP, 2)
        gates_here = lax.dynamic_slice_in_dim(gate_of, start, CAP, 2)
        picked = jax.vmap(jax.vmap(pick_rows))(grads_blocks, tokens_here)
        routed = to_half(picked.astype(jnp.float32) * gates_here[..., None]).reshape(N_DP, SLOTS, D)
        hidden_here = lax.dynamic_index_in_dim(hidden_acts, expert_num, 1, keepdims=False)
        q_here = lax.dynamic_index_in_dim(q_previous, expert_num, 0, keepdims=False)
        mixed = to_half(jnp.einsum('psd,rd->psr', routed.astype(jnp.float32), q_here.astype(jnp.float32)))
        factor = jnp.einsum('psr,psf->rf', mixed.astype(jnp.float32), hidden_here.astype(jnp.float32))
        gram = jnp.dot(factor, factor.T, precision=lax.Precision.HIGHEST)
        lower = jnp.linalg.cholesky(gram)
        inverse = jax.scipy.linalg.solve_triangular(lower, jnp.eye(RANK, dtype=jnp.float32), lower=True)
        ortho = jnp.dot(inverse, factor, precision=lax.Precision.HIGHEST)
        ortho_half = to_half(ortho)
        projected = to_half(jnp.einsum('psf,rf->psr', hidden_here.astype(jnp.float32), ortho_half.astype(jnp.float32)))
        q_new = jnp.einsum('psr,psd->rd', projected.astype(jnp.float32), routed.astype(jnp.float32))
        return (ortho * math.sqrt(FF), q_new)
    new_basis, q_update = lax.map(one_expert, jnp.arange(EXPERTS, dtype=jnp.int32))
    return (new_basis, q_update)
```

```python
import math

import jax
import jax.numpy as jnp
from jax import lax
from jax.experimental import pallas as pl
from jax.experimental.pallas import tpu as pltpu
from jax.sharding import Mesh, PartitionSpec as P

F32 = jnp.float32
BF16 = jnp.bfloat16
HIGHEST = lax.Precision.HIGHEST
NN = (((1,), (0,)), ((), ()))
NT = (((1,), (1,)), ((), ()))
CP = 8


def params(limit_mib=48, **kw):
    return pltpu.CompilerParams(vmem_limit_bytes=limit_mib * 2**20, **kw)


def table_kernel(ids_ref, gates_ref, out_ref):
    ids = ids_ref[...]
    gates = gates_ref[...]
    tokens, top = ids.shape
    shape = (tokens, 256)
    lane = lax.broadcasted_iota(jnp.int32, shape, 1)
    rem = lane % 128
    expert = 16 * (rem // 8) + 8 * (lane // 128) + rem % 8
    hit = jnp.zeros(shape, F32)
    gate = jnp.zeros(shape, F32)
    for k in range(top):
        same = ids[:, k : k + 1] == expert
        hit = jnp.where(same, 1.0, hit)
        gate = jnp.where(same, gates[:, k : k + 1], gate)
    row = lax.broadcasted_iota(jnp.int32, (tokens, tokens), 0)
    col = lax.broadcasted_iota(jnp.int32, (tokens, tokens), 1)
    before = jnp.where(col < row, 1.0, 0.0).astype(BF16)
    pos = lax.dot_general(before, hit.astype(BF16), NN, preferred_element_type=F32)
    code = lax.broadcasted_iota(jnp.int32, shape, 0).astype(F32) + gate
    code = jnp.where(hit > 0, code, -1.0)
    for c in range(CP):
        picked = jnp.max(jnp.where(pos == c, code, -1.0), axis=0, keepdims=True)
        out_ref[0, c : c + 1, :] = picked[:, :128]
        out_ref[1, c : c + 1, :] = picked[:, 128:]


def slot_codes(ids, gates):
    return pl.pallas_call(
        table_kernel,
        out_shape=jax.ShapeDtypeStruct((2, CP, 128), F32),
        name="slot_codes",
    )(ids, gates)


def dispatch_kernel(core_ref, codes_ref, xt_ref, out_ref):
    token = lax.broadcasted_iota(jnp.int32, (CP, 128), 1).astype(F32)
    group = 32
    for g in range(128 // group):
        rows = []
        for i in range(2):
            code = codes_ref[i, 0]
            parts = []
            for x in range(g * group, (g + 1) * group):
                u = code[:, x : x + 1] - token
                parts.append(jnp.where((u > 0) & (u < 1), u, 0.0))
            picks = jnp.concatenate(parts, axis=0).astype(BF16)
            got = lax.dot_general(picks, xt_ref[i], NT, preferred_element_type=F32)
            rows.append(got.reshape(group, CP, got.shape[1]))
        out_ref[g * group : (g + 1) * group] = jnp.concatenate(rows, axis=1).astype(BF16)


def dispatch(core, codes, xt, half):
    chips, width, tokens = xt.shape

    def code_map(i, core_ref):
        c = core_ref[0]
        return (i, c if half == 0 else 1 - c, 0, 0)

    return pl.pallas_call(
        dispatch_kernel,
        grid_spec=pltpu.PrefetchScalarGridSpec(
            num_scalar_prefetch=1,
            grid=(chips // 2,),
            in_specs=[
                pl.BlockSpec((2, 1, CP, 128), code_map),
                pl.BlockSpec((2, width, tokens), lambda i, _: (i, 0, 0)),
            ],
            out_specs=pl.BlockSpec((128, 2 * CP, width), lambda i, _: (0, i, 0)),
        ),
        out_shape=jax.ShapeDtypeStruct((128, chips * CP, width), BF16),
        compiler_params=params(),
        cost_estimate=pl.CostEstimate(
            flops=2 * 128 * CP * chips * tokens * width, bytes_accessed=128 * chips * CP * width * 2, transcendentals=0
        ),
        name="dispatch",
    )(core, codes, xt)


def mix_kernel(core_ref, own_ref, sib_ref, qt_ref, out_ref, tmp_ref):
    core = core_ref[0]
    owner = lax.broadcasted_iota(jnp.int32, (128, 256), 1) // 32
    for half, ref in enumerate((own_ref, sib_ref)):
        experts, rows, width = ref.shape
        got = lax.dot_general(
            ref[...].reshape(experts * rows, width), qt_ref[0], NN, preferred_element_type=F32
        )
        acc = got[:rows]
        for x in range(1, experts):
            acc = jnp.where(owner == x, got[x * rows : (x + 1) * rows], acc)
        place = core if half == 0 else 1 - core
        for i in range(2):
            lanes = slice(i * 128, (i + 1) * 128)
            tmp_ref[i] = acc[:, lanes]
            for c in range(6):
                out_ref[0, c, place, :, lanes] = tmp_ref[i, pl.ds(c, 16, stride=CP), :].astype(BF16)


def mix(core, own, sib, qt):
    chips = qt.shape[0]
    width = own.shape[2]
    block = pl.BlockSpec((8, 128, width), lambda i, _: (i, 0, 0))
    return pl.pallas_call(
        mix_kernel,
        grid_spec=pltpu.PrefetchScalarGridSpec(
            num_scalar_prefetch=1,
            grid=(chips,),
            in_specs=[block, block, pl.BlockSpec((1, width, 256), lambda i, _: (i, 0, 0))],
            out_specs=pl.BlockSpec((1, 6, 2, 16, 256), lambda i, _: (i, 0, 0, 0, 0)),
            scratch_shapes=[pltpu.VMEM((2, 128, 128), F32)],
        ),
        out_shape=jax.ShapeDtypeStruct((chips, 6, 2, 16, 256), BF16),
        compiler_params=params(),
        cost_estimate=pl.CostEstimate(
            flops=2 * 128 * 256 * width * 256, bytes_accessed=128 * 256 * width * 2, transcendentals=0
        ),
        name="mix",
    )(core, own, sib, qt)


def factor_kernel(parts_ref, hidden_ref, out_ref, tmp_ref, lhs_ref):
    x = pl.program_id(0)

    @pl.when(x == 0)
    def _():
        for c in range(6):
            for k in range(2):
                total = parts_ref[0, c, k].astype(F32)
                for j in range(1, parts_ref.shape[0]):
                    total = total + parts_ref[j, c, k].astype(F32)
                for i in range(2):
                    tmp_ref[i, pl.ds(k * 6 + c, 16, stride=12), :] = total[:, i * 128 : (i + 1) * 128]
        for i in range(2):
            lhs_ref[i * 128 : (i + 1) * 128] = tmp_ref[i].T

    start = pl.multiple_of(x * 32, 32)
    lhs = lhs_ref[pl.ds(start, 32), 0:192].astype(BF16)
    out_ref[0] = lax.dot_general(lhs, hidden_ref[0], NN, preferred_element_type=F32).astype(BF16)


def first_factor(parts, hidden):
    experts, slots, units = hidden.shape
    return pl.pallas_call(
        factor_kernel,
        grid=(experts,),
        in_specs=[
            pl.BlockSpec(parts.shape, lambda i: (0, 0, 0, 0, 0)),
            pl.BlockSpec((1, slots, units), lambda i: (i, 0, 0)),
        ],
        out_specs=pl.BlockSpec((1, 32, units), lambda i: (i, 0, 0)),
        out_shape=jax.ShapeDtypeStruct((experts, 32, units), BF16),
        scratch_shapes=[pltpu.VMEM((2, 256, 128), F32), pltpu.VMEM((256, 256), F32)],
        compiler_params=params(),
        name="first_factor",
    )(parts, hidden)


def ortho_kernel(parts_ref, out_ref):
    count = parts_ref.shape[1]
    factors, systems = [], []
    row = lax.broadcasted_iota(jnp.int32, (32, 32), 0)
    col = lax.broadcasted_iota(jnp.int32, (32, 32), 1)
    eye = jnp.where(row == col, 1.0, 0.0)
    for m in range(count):
        value = parts_ref[0, m].astype(F32)
        for p in range(1, parts_ref.shape[0]):
            value = value + parts_ref[p, m].astype(F32)
        factors.append(value)
        gram = lax.dot_general(value, value, NT, precision=HIGHEST, preferred_element_type=F32)
        systems.append(jnp.concatenate([gram, eye], axis=1))
    index = lax.broadcasted_iota(jnp.int32, (32, 64), 0)
    for k in range(32):
        for m in range(count):
            a = systems[m]
            inv = lax.rsqrt(a[k : k + 1, k : k + 1])
            pivot = a[k : k + 1, :] * inv
            lower = a[:, k : k + 1] * inv
            below = a - lower * pivot
            systems[m] = jnp.where(index > k, below, jnp.where(index == k, pivot, a))
    for m in range(count):
        inverse = systems[m][:, 32:]
        out_ref[m] = lax.dot_general(
            inverse, factors[m], NN, precision=HIGHEST, preferred_element_type=F32
        ).astype(BF16)


def ortho_of(parts):
    _, count, rank, units = parts.shape
    return pl.pallas_call(
        ortho_kernel,
        out_shape=jax.ShapeDtypeStruct((count, rank, units), BF16),
        compiler_params=params(),
        name="ortho",
    )(parts)


def project_kernel(ortho_ref, hidden_ref, basis_ref, out_ref, tmp_ref, rows_ref):
    x = pl.program_id(0)
    ortho = ortho_ref[0]
    basis_ref[0] = ortho.astype(F32) * math.sqrt(ortho.shape[1])
    got = lax.dot_general(ortho, hidden_ref[0], NT, preferred_element_type=F32)
    start = pl.multiple_of(x * 32, 32)
    tmp_ref[pl.ds(start, 32), 0:192] = got

    @pl.when(x == pl.num_programs(0) - 1)
    def _():
        for i in range(2):
            rows_ref[i] = tmp_ref[i * 128 : (i + 1) * 128, :].T
            for c in range(6):
                for k in range(2):
                    out_ref[c, k, :, i * 128 : (i + 1) * 128] = rows_ref[
                        i, pl.ds(k * 6 + c, 16, stride=12), :
                    ].astype(BF16)


def project(ortho, hidden):
    experts, slots, units = hidden.shape
    return pl.pallas_call(
        project_kernel,
        grid=(experts,),
        in_specs=[
            pl.BlockSpec((1, 32, units), lambda i: (i, 0, 0)),
            pl.BlockSpec((1, slots, units), lambda i: (i, 0, 0)),
        ],
        out_specs=[
            pl.BlockSpec((1, 32, units), lambda i: (i, 0, 0)),
            pl.BlockSpec((6, 2, 16, 256), lambda i: (0, 0, 0, 0)),
        ],
        out_shape=[
            jax.ShapeDtypeStruct((experts, 32, units), F32),
            jax.ShapeDtypeStruct((6, 2, 16, 256), BF16),
        ],
        scratch_shapes=[pltpu.VMEM((256, 256), F32), pltpu.VMEM((2, 256, 128), F32)],
        compiler_params=params(),
        name="project",
    )(ortho, hidden)


def terms_kernel(core_ref, own_ref, sib_ref, proj_ref, out_ref, rows_ref, sum_ref):
    core = core_ref[0]
    experts, rows, width = own_ref.shape

    @pl.when(pl.program_id(0) == 0)
    def _():
        rows_ref[...] = jnp.zeros_like(rows_ref)
        sum_ref[...] = jnp.zeros_like(sum_ref)

    for half in range(2):
        place = core if half == 0 else 1 - core
        for c in range(6):
            values = proj_ref[0, c, place].astype(F32)
            for i in range(2):
                rows_ref[i, pl.ds(half * 128 + c, 16, stride=CP), :] = values[:, i * 128 : (i + 1) * 128]
    turned = [rows_ref[i].T.astype(BF16) for i in range(2)]
    for x in range(experts):
        at = (x % 4) * 32
        lhs = turned[x // 4][at : at + 32]
        got = lax.dot_general(lhs[:, :128], own_ref[x], NN, preferred_element_type=F32)
        got = got + lax.dot_general(lhs[:, 128:], sib_ref[x], NN, preferred_element_type=F32)
        sum_ref[x * 32 : (x + 1) * 32, 0:width] = got
    for i in range(4):
        turned = sum_ref[:, i * 128 : (i + 1) * 128].T
        tall = min(width - i * 128, 128)
        rows_out = turned[:tall].astype(BF16)
        done = 0
        while done < tall:
            at = i * 128 + done
            part, offset = divmod(at, width // 4)
            step = min(tall - done, width // 4 - offset)
            out_ref[part, 0, offset : offset + step, :] = rows_out[done : done + step]
            done += step


def second_terms(core, own, sib, proj):
    chips = proj.shape[0]
    width = own.shape[2]
    block = pl.BlockSpec((8, 128, width), lambda i, _: (i, 0, 0))
    return pl.pallas_call(
        terms_kernel,
        grid_spec=pltpu.PrefetchScalarGridSpec(
            num_scalar_prefetch=1,
            grid=(chips,),
            in_specs=[block, block, pl.BlockSpec((1, 6, 2, 16, 256), lambda i, _: (i, 0, 0, 0, 0))],
            out_specs=pl.BlockSpec((4, 1, width // 4, 256), lambda i, _: (0, i, 0, 0)),
            scratch_shapes=[pltpu.VMEM((2, 256, 128), F32), pltpu.VMEM((256, 512), F32)],
        ),
        out_shape=jax.ShapeDtypeStruct((4, chips, width // 4, 256), BF16),
        compiler_params=params(),
        name="second_terms",
    )(core, own, sib, proj)


def gather_kernel(parts_ref, out_ref):
    total = parts_ref[0].astype(F32)
    for p in range(1, parts_ref.shape[0]):
        total = total + parts_ref[p].astype(F32)
    out_ref[...] = total.T


def owned_columns(parts):
    copies, columns, rows = parts.shape
    return pl.pallas_call(
        gather_kernel,
        grid=(columns // 128,),
        in_specs=[pl.BlockSpec((copies, 128, rows), lambda i: (0, i, 0))],
        out_specs=pl.BlockSpec((rows, 128), lambda i: (0, i)),
        out_shape=jax.ShapeDtypeStruct((rows, columns), F32),
        name="owned_columns",
    )(parts)


def exchange(values, axes):
    return lax.all_to_all(values, axes, split_axis=0, concat_axis=0, tiled=True)


def for_chips(turned, chips, copies):
    columns, lanes = turned.shape
    cut = turned.reshape(copies, chips, columns // (copies * chips), lanes)
    return jnp.swapaxes(cut, 0, 1).reshape(chips, columns // chips, lanes)


def local(out_grads, expert_ids, gate_probs, hidden_acts, q_previous):
    chips = lax.axis_size("chip")
    copies = lax.axis_size("dp")
    core = lax.axis_index("core").astype(jnp.int32).reshape(1)
    hidden = hidden_acts[0]
    experts, rank, width = q_previous.shape
    units = hidden.shape[2]

    codes = slot_codes(expert_ids[0], gate_probs[0])
    codes = jnp.broadcast_to(codes[None], (chips, *codes.shape)).reshape(2 * chips, CP, 128)
    codes = exchange(codes, ("chip", "core")).reshape(chips, 2, CP, 128)

    own_t = exchange(for_chips(out_grads[0].T, chips, copies), "chip")
    sib_t = lax.ppermute(own_t, "core", [(0, 1), (1, 0)])
    q_t = for_chips(q_previous.reshape(experts * rank, width).T, chips, copies)
    q_t = exchange(q_t, "chip")

    own = dispatch(core, codes, own_t, 0)
    sib = dispatch(core, codes, sib_t, 1)
    mixed = exchange(mix(core, own, sib, q_t), "chip")
    factor = first_factor(mixed, hidden)
    factor = exchange(factor, "dp").reshape(copies, experts // copies, rank, units)
    ortho = ortho_of(factor)
    ortho = exchange(jnp.broadcast_to(ortho[None], (copies, *ortho.shape)), "dp")
    ortho = ortho.reshape(experts, rank, units)
    new_basis, proj = project(ortho, hidden)
    proj = exchange(jnp.broadcast_to(proj[None], (chips, *proj.shape)), "chip")
    terms = second_terms(core, own, sib, proj)
    terms = terms.reshape(copies * chips, -1, experts * rank)
    terms = exchange(terms, ("dp", "chip")).reshape(copies, width // copies, experts * rank)
    q_update = owned_columns(terms).reshape(experts, rank, width // copies)
    return (new_basis, q_update)


def solution(mesh):
    at = mesh.axis_names.index("expert")
    shape = mesh.devices.shape
    devices = mesh.devices.reshape(*shape[:at], shape[at] // 2, 2, *shape[at + 1 :])
    names = (*mesh.axis_names[:at], "chip", "core", *mesh.axis_names[at + 1 :])
    expert = ("chip", "core")
    return jax.shard_map(
        local,
        mesh=Mesh(devices, names),
        in_specs=(
            P("dp", expert, None),
            P("dp", expert, None),
            P("dp", expert, None),
            P("dp", expert, None, None),
            P(expert, None, None),
        ),
        out_specs=(P(expert, None, None), P(expert, None, "dp")),
        check_vma=False,
    )
```

```python
import math

import jax
import jax.numpy as jnp
from jax import lax
from jax.experimental import pallas as pl
from jax.experimental.pallas import tpu as pltpu
from jax.sharding import Mesh, PartitionSpec as P

F32 = jnp.float32
BF16 = jnp.bfloat16
HIGHEST = lax.Precision.HIGHEST
NN = (((1,), (0,)), ((), ()))
NT = (((1,), (1,)), ((), ()))
CP = 8
CAP = 6
STREAMS = 2


def params(limit_mib=48, **kw):
    return pltpu.CompilerParams(vmem_limit_bytes=limit_mib * 2**20, **kw)


def shape_of(shape, dtype):
    return jax.ShapeDtypeStruct(shape, dtype)


def place_rows(out_ref, turned, first, part_rows, base):
    done = 0
    while done < turned.shape[0]:
        chip, offset = divmod(first + done, part_rows)
        step = min(turned.shape[0] - done, part_rows - offset)
        out_ref[chip, base + offset : base + offset + step, :] = turned[done : done + step]
        done += step


def prepare_kernel(ids_ref, gates_ref, grads_ref, out_ref):
    ids = ids_ref[...].T
    gates = gates_ref[...].T
    chips, total, _ = out_ref.shape
    tokens, top = ids.shape
    width = grads_ref.shape[1]
    shape = (tokens, 256)
    lane = lax.broadcasted_iota(jnp.int32, shape, 1)
    rem = lane % 128
    expert = 16 * (rem // 8) + 8 * (lane // 128) + rem % 8
    hit = jnp.zeros(shape, F32)
    gate = jnp.zeros(shape, F32)
    for k in range(top):
        same = ids[:, k : k + 1] == expert
        hit = jnp.where(same, 1.0, hit)
        gate = jnp.where(same, gates[:, k : k + 1], gate)
    row = lax.broadcasted_iota(jnp.int32, (tokens, tokens), 0)
    col = lax.broadcasted_iota(jnp.int32, (tokens, tokens), 1)
    before = jnp.where(col < row, 1.0, 0.0).astype(BF16)
    pos = lax.dot_general(before, hit.astype(BF16), NN, preferred_element_type=F32)
    pos = jnp.where(hit > 0, pos, -1.0)
    token = lax.broadcasted_iota(jnp.int32, shape, 0).astype(F32)
    token_rows, gate_rows = [], []
    for c in range(CP):
        here = pos == c
        token_rows.append(jnp.max(jnp.where(here, token, -1.0), axis=0, keepdims=True))
        gate_rows.append(jnp.sum(jnp.where(here, gate, 0.0), axis=0, keepdims=True))
    table = jnp.concatenate(token_rows + gate_rows, axis=0).astype(BF16)
    table = jnp.concatenate([table[:, :128], table[:, 128:]], axis=0)
    codes_at = total - 4 * CP
    for j in range(chips):
        out_ref[j, codes_at:, :] = table
    copies = 4
    span = width // copies
    part = span // chips
    for p in range(copies):
        for n in range(span // 128):
            turned = grads_ref[:, p * span + n * 128 : p * span + (n + 1) * 128].T
            place_rows(out_ref, turned, n * 128, part, p * part)


def prepare(ids, gates, grads, chips):
    tokens, width = grads.shape
    return pl.pallas_call(
        prepare_kernel,
        out_shape=shape_of((chips, width // chips + 4 * CP, tokens), BF16),
        compiler_params=params(),
        name="prepare",
    )(ids.T, gates.T, grads)


def turn_kernel(copy_ref, q_ref, out_ref):
    for n in range(q_ref.shape[1] // 128):
        out_ref[n * 128 : (n + 1) * 128, :] = q_ref[:, n * 128 : (n + 1) * 128].T


def turned_part(copy, q, copies):
    rows, width = q.shape
    steps = 2
    columns = width // copies
    return pl.pallas_call(
        turn_kernel,
        grid_spec=pltpu.PrefetchScalarGridSpec(
            num_scalar_prefetch=1,
            grid=(steps,),
            in_specs=[pl.BlockSpec((rows, columns // steps), lambda i, c: (0, c[0] * steps + i))],
            out_specs=pl.BlockSpec((columns // steps, rows), lambda i, c: (i, 0)),
        ),
        out_shape=shape_of((columns, rows), BF16),
        compiler_params=params(),
        name="turned_part",
    )(copy, q)


def dispatch_kernel(core_ref, xt_ref, out_ref, *, half):
    core = core_ref[0]
    token = lax.broadcasted_iota(jnp.int32, (CP, 128), 1).astype(F32)
    group = 32
    width = out_ref.shape[2]
    start = pl.multiple_of(width + 2 * CP * core, 2 * CP)
    codes = []
    for i in range(2):
        table = xt_ref[i, pl.ds(start, 2 * CP), :].astype(F32)
        codes.append(table[:CP] + table[CP:])
    for g in range(128 // group):
        rows = []
        for i in range(2):
            parts = []
            for x in range(g * group, (g + 1) * group):
                u = codes[i][:, x : x + 1] - token
                parts.append(jnp.where((u > 0) & (u < 1), u, 0.0))
            picks = jnp.concatenate(parts, axis=0).astype(BF16)
            got = lax.dot_general(picks, xt_ref[i, :width], NT, preferred_element_type=F32)
            rows.append(got.reshape(group, CP, width))
        out_ref[g * group : (g + 1) * group] = jnp.concatenate(rows, axis=1).astype(BF16)


def dispatch(core, xt, half):
    chips, total, tokens = xt.shape
    width = total - 4 * CP

    def body(*refs):
        dispatch_kernel(*refs, half=half)

    return pl.pallas_call(
        body,
        grid_spec=pltpu.PrefetchScalarGridSpec(
            num_scalar_prefetch=1,
            grid=(chips // 2,),
            in_specs=[pl.BlockSpec((2, total, tokens), lambda i, _: (i, 0, 0))],
            out_specs=pl.BlockSpec((128, 2 * CP, width), lambda i, _: (0, i, 0)),
        ),
        out_shape=shape_of((128, chips * CP, width), BF16),
        compiler_params=params(),
        cost_estimate=pl.CostEstimate(
            flops=2 * 128 * CP * chips * tokens * width, bytes_accessed=128 * chips * CP * width * 2, transcendentals=0
        ),
        name=f"dispatch_{half}",
    )(core, xt)


def mix_kernel(at_ref, own_ref, sib_ref, *rest):
    q_refs, (out_ref, q_ref, tmp_ref) = rest[:-3], rest[-3:]
    core, copy = at_ref[0], at_ref[1]
    copies = len(q_refs)
    lanes = out_ref.shape[4]
    owner = lax.broadcasted_iota(jnp.int32, (128, lanes), 1) // 32
    for n in range(out_ref.shape[0]):
        part = q_refs[0].shape[1]
        for shift, ref in enumerate(q_refs):
            start = pl.multiple_of(part * ((copy + shift) % copies), 16)
            q_ref[pl.ds(start, part), :] = ref[n]
        for half, ref in enumerate((own_ref, sib_ref)):
            _, experts, rows, width = ref.shape
            got = lax.dot_general(
                ref[n].reshape(experts * rows, width), q_ref[...], NN, preferred_element_type=F32
            )
            acc = got[:rows]
            for x in range(1, experts):
                acc = jnp.where(owner == x, got[x * rows : (x + 1) * rows], acc)
            tmp_ref[...] = acc
            place = core if half == 0 else 1 - core
            for c in range(CAP):
                out_ref[n, c, place] = tmp_ref[pl.ds(c, 16, stride=CP), :].astype(BF16)


def mix(at, own, sib, q_parts, stream):
    chips, part, lanes = q_parts[0].shape
    lanes = lanes // STREAMS
    _, experts, rows, width = own.shape
    experts = experts // STREAMS
    step = 2
    block = pl.BlockSpec((step, experts, rows, width), lambda i, _: (i, stream, 0, 0))
    q_block = pl.BlockSpec((step, part, lanes), lambda i, _: (i, 0, stream))
    return pl.pallas_call(
        mix_kernel,
        grid_spec=pltpu.PrefetchScalarGridSpec(
            num_scalar_prefetch=1,
            grid=(chips // step,),
            in_specs=[block, block] + [q_block] * len(q_parts),
            out_specs=pl.BlockSpec((step, CAP, 2, 16, lanes), lambda i, _: (i, 0, 0, 0, 0)),
            scratch_shapes=[pltpu.VMEM((width, lanes), BF16), pltpu.VMEM((rows, lanes), F32)],
        ),
        out_shape=shape_of((chips, CAP, 2, 16, lanes), BF16),
        compiler_params=params(),
        cost_estimate=pl.CostEstimate(
            flops=4 * chips * experts * rows * width * 256,
            bytes_accessed=4 * chips * experts * rows * width,
            transcendentals=0,
        ),
        name=f"mix_{stream}",
    )(at, own, sib, *q_parts)


def factor_kernel(parts_ref, hidden_ref, out_ref, tmp_ref, lhs_ref):
    step = pl.program_id(0)
    here = hidden_ref.shape[0]

    @pl.when(step == 0)
    def _():
        for c in range(CAP):
            for k in range(2):
                total = parts_ref[0, c, k].astype(F32)
                for j in range(1, parts_ref.shape[0]):
                    total = total + parts_ref[j, c, k].astype(F32)
                tmp_ref[pl.ds(k * CAP + c, 16, stride=2 * CAP), :] = total
        lhs_ref[...] = tmp_ref[...].T.astype(BF16)

    for n in range(here):
        start = pl.multiple_of((step * here + n) * 32, 32)
        lhs = lhs_ref[pl.ds(start, 32), 0 : hidden_ref.shape[1]]
        out_ref[n] = lax.dot_general(lhs, hidden_ref[n], NN, preferred_element_type=F32).astype(BF16)


def first_factor(parts, hidden, stream):
    experts, slots, units = hidden.shape
    experts = experts // STREAMS
    lanes = parts.shape[4]
    step = 2
    first = stream * experts // step
    return pl.pallas_call(
        factor_kernel,
        grid=(experts // step,),
        in_specs=[
            pl.BlockSpec(parts.shape, lambda i: (0, 0, 0, 0, 0)),
            pl.BlockSpec((step, slots, units), lambda i: (first + i, 0, 0)),
        ],
        out_specs=pl.BlockSpec((step, 32, units), lambda i: (i, 0, 0)),
        out_shape=shape_of((experts, 32, units), BF16),
        scratch_shapes=[pltpu.VMEM((256, lanes), F32), pltpu.VMEM((lanes, 256), BF16)],
        compiler_params=params(),
        cost_estimate=pl.CostEstimate(
            flops=2 * experts * slots * units * 256, bytes_accessed=2 * experts * slots * units, transcendentals=0
        ),
        name=f"first_factor_{stream}",
    )(parts, hidden)


def ortho_kernel(parts_ref, out_ref):
    count = parts_ref.shape[1]
    factors, systems = [], []
    row = lax.broadcasted_iota(jnp.int32, (32, 32), 0)
    col = lax.broadcasted_iota(jnp.int32, (32, 32), 1)
    eye = jnp.where(row == col, 1.0, 0.0)
    for m in range(count):
        value = parts_ref[0, m].astype(F32)
        for p in range(1, parts_ref.shape[0]):
            value = value + parts_ref[p, m].astype(F32)
        factors.append(value)
        gram = lax.dot_general(value, value, NT, precision=HIGHEST, preferred_element_type=F32)
        systems.append(jnp.concatenate([gram, eye], axis=1))
    index = lax.broadcasted_iota(jnp.int32, (32, 64), 0)
    for k in range(32):
        for m in range(count):
            a = systems[m]
            inv = lax.rsqrt(a[k : k + 1, k : k + 1])
            pivot = a[k : k + 1, :] * inv
            lower = a[:, k : k + 1] * inv
            below = a - lower * pivot
            systems[m] = jnp.where(index > k, below, jnp.where(index == k, pivot, a))
    for m in range(count):
        inverse = systems[m][:, 32:]
        out_ref[m] = lax.dot_general(
            inverse, factors[m], NN, precision=HIGHEST, preferred_element_type=F32
        ).astype(BF16)


def ortho_of(parts, stream):
    _, count, rank, units = parts.shape
    return pl.pallas_call(
        ortho_kernel,
        out_shape=shape_of((count, rank, units), BF16),
        compiler_params=params(),
        cost_estimate=pl.CostEstimate(flops=5_000_000_000, bytes_accessed=4 * rank * units * 2, transcendentals=0),
        name=f"ortho_{stream}",
    )(parts)


def project_kernel(ortho_ref, hidden_ref, *refs):
    basis_ref, out_ref, rows_ref = refs[-3:]
    step = pl.program_id(0)
    here, slots, units = hidden_ref.shape
    start = pl.multiple_of(step * here * 32, 32)
    basis = ortho_ref[pl.ds(start, here * 32), :].astype(F32) * math.sqrt(units)
    basis_ref[...] = basis.reshape(here, 32, units)
    got = lax.dot_general(
        hidden_ref[...].reshape(here * slots, units), ortho_ref[...], NT, preferred_element_type=F32
    )
    owner = lax.broadcasted_iota(jnp.int32, (slots, ortho_ref.shape[0]), 1) // 32
    for n in range(here):
        value = got[n * slots : (n + 1) * slots]
        kept = rows_ref[...]
        rows_ref[...] = jnp.where(owner == step * here + n, value, kept)

    @pl.when(step == pl.num_programs(0) - 1)
    def _():
        for c in range(CAP):
            for k in range(2):
                out_ref[c, k] = rows_ref[pl.ds(k * CAP + c, 16, stride=2 * CAP), :].astype(BF16)


def project(ortho, hidden, stream, basis):
    every, slots, units = hidden.shape
    experts = every // STREAMS
    lanes = experts * 32
    step = 2
    first = stream * experts // step
    given = [] if basis is None else [basis]
    return pl.pallas_call(
        project_kernel,
        grid=(experts // step,),
        in_specs=[
            pl.BlockSpec((lanes, units), lambda i: (0, 0)),
            pl.BlockSpec((step, slots, units), lambda i: (first + i, 0, 0)),
        ]
        + [pl.BlockSpec(memory_space=pl.ANY)] * len(given),
        out_specs=[
            pl.BlockSpec((step, 32, units), lambda i: (first + i, 0, 0)),
            pl.BlockSpec((CAP, 2, 16, lanes), lambda i: (0, 0, 0, 0)),
        ],
        out_shape=[
            shape_of((every, 32, units), F32),
            shape_of((CAP, 2, 16, lanes), BF16),
        ],
        input_output_aliases={2: 0} if given else {},
        scratch_shapes=[pltpu.VMEM((slots, lanes), F32)],
        compiler_params=params(),
        cost_estimate=pl.CostEstimate(
            flops=2 * experts * slots * units * 256, bytes_accessed=2 * experts * slots * units, transcendentals=0
        ),
        name=f"project_{stream}",
    )(ortho, hidden, *given)


def terms_kernel(core_ref, own_ref, sib_ref, proj_ref, out_ref, rows_ref, sum_ref):
    core = core_ref[0]
    count, experts, rows, width = own_ref.shape
    part = width // 4

    @pl.when(pl.program_id(0) == 0)
    def _():
        rows_ref[...] = jnp.zeros_like(rows_ref)
        sum_ref[...] = jnp.zeros_like(sum_ref)

    for n in range(count):
        for half in range(2):
            place = core if half == 0 else 1 - core
            for c in range(CAP):
                rows_ref[pl.ds(half * 128 + c, 16, stride=CP), :] = proj_ref[n, c, place].astype(F32)
        turned = rows_ref[...].T.astype(BF16)
        for x in range(experts):
            both = jnp.concatenate([own_ref[n, x], sib_ref[n, x]], axis=0)
            got = lax.dot_general(turned[x * 32 : (x + 1) * 32], both, NN, preferred_element_type=F32)
            sum_ref[x * 32 : (x + 1) * 32, 0:width] = got
        for i in range(4):
            tall = min(width - i * 128, 128)
            back = sum_ref[:, i * 128 : (i + 1) * 128].T[:tall].astype(BF16)
            done = 0
            while done < tall:
                p, offset = divmod(i * 128 + done, part)
                step = min(tall - done, part - offset)
                out_ref[p, n, offset : offset + step, :] = back[done : done + step]
                done += step


def second_terms(core, own, sib, proj, stream):
    chips, _, _, _, lanes = proj.shape
    _, experts, rows, width = own.shape
    experts = experts // STREAMS
    step = 2
    block = pl.BlockSpec((step, experts, rows, width), lambda i, _: (i, stream, 0, 0))
    return pl.pallas_call(
        terms_kernel,
        grid_spec=pltpu.PrefetchScalarGridSpec(
            num_scalar_prefetch=1,
            grid=(chips // step,),
            in_specs=[block, block, pl.BlockSpec((step, CAP, 2, 16, lanes), lambda i, _: (i, 0, 0, 0, 0))],
            out_specs=pl.BlockSpec((4, step, width // 4, lanes), lambda i, _: (0, i, 0, 0)),
            scratch_shapes=[pltpu.VMEM((256, lanes), F32), pltpu.VMEM((lanes, 512), F32)],
        ),
        out_shape=shape_of((4, chips, width // 4, lanes), BF16),
        compiler_params=params(),
        cost_estimate=pl.CostEstimate(
            flops=4 * chips * experts * rows * width * 256,
            bytes_accessed=4 * chips * experts * rows * width,
            transcendentals=0,
        ),
        name=f"second_terms_{stream}",
    )(core, own, sib, proj)


def gather_kernel(parts_ref, *refs):
    out_ref = refs[-1]
    total = parts_ref[0].astype(F32)
    for p in range(1, parts_ref.shape[0]):
        total = total + parts_ref[p].astype(F32)
    out_ref[...] = total.T


def owned_columns(parts, stream, sums):
    copies, columns, rows = parts.shape
    given = [] if sums is None else [sums]
    wide = 896
    return pl.pallas_call(
        gather_kernel,
        grid=(columns // wide,),
        in_specs=[pl.BlockSpec((copies, wide, rows), lambda i: (0, i, 0))]
        + [pl.BlockSpec(memory_space=pl.ANY)] * len(given),
        out_specs=pl.BlockSpec((rows, wide), lambda i: (stream, i)),
        out_shape=shape_of((rows * STREAMS, columns), F32),
        input_output_aliases={1: 0} if given else {},
        compiler_params=params(),
        name=f"owned_columns_{stream}",
    )(parts, *given)


def exchange(values, axes):
    return lax.all_to_all(values, axes, split_axis=0, concat_axis=0, tiled=True)


def to_all(values, axis):
    return exchange(jnp.broadcast_to(values[None], (lax.axis_size(axis), *values.shape)), axis)


def around(part, copies):
    ahead = [(i, (i + 1) % copies) for i in range(copies)]
    back = [(i, (i - 1) % copies) for i in range(copies)]
    half = part.shape[0] // 2
    before = lax.ppermute(part, "dp", ahead)
    after = lax.ppermute(part, "dp", back)
    far_low = lax.ppermute(before[:half], "dp", ahead)
    far_high = lax.ppermute(after[half:], "dp", back)
    return [part, after, jnp.concatenate([far_low, far_high], axis=0), before]


def local(out_grads, expert_ids, gate_probs, hidden_acts, q_previous):
    chips = lax.axis_size("chip")
    copies = lax.axis_size("dp")
    core = lax.axis_index("core").astype(jnp.int32).reshape(1)
    copy = lax.axis_index("dp").astype(jnp.int32).reshape(1)
    at = jnp.concatenate([core, copy])
    hidden = hidden_acts[0]
    experts, rank, width = q_previous.shape
    units = hidden.shape[2]
    here = experts // STREAMS

    q_part = turned_part(copy, q_previous.reshape(experts * rank, width), copies)
    q_part = exchange(q_part.reshape(chips, -1, experts * rank), "chip")
    q_parts = around(q_part, copies)

    own_t = exchange(prepare(expert_ids[0], gate_probs[0], out_grads[0], chips), "chip")
    sib_t = lax.ppermute(own_t, "core", [(0, 1), (1, 0)])
    own = dispatch(core, own_t, 0)
    sib = dispatch(core, sib_t, 1)
    own = own.reshape(chips, experts, *own.shape[1:])
    sib = sib.reshape(chips, experts, *sib.shape[1:])

    basis, sums = None, None
    for s in range(STREAMS):
        mixed = exchange(mix(at, own, sib, q_parts, s), "chip")
        factor = exchange(first_factor(mixed, hidden, s), "dp")
        ortho = ortho_of(factor.reshape(copies, here // copies, rank, units), s)
        ortho = to_all(ortho, "dp").reshape(here * rank, units)
        basis, proj = project(ortho, hidden, s, basis)
        terms = second_terms(core, own, sib, to_all(proj, "chip"), s)
        terms = exchange(terms.reshape(copies * chips, -1, here * rank), ("dp", "chip"))
        sums = owned_columns(terms.reshape(copies, width // copies, here * rank), s, sums)
    return (basis, sums.reshape(experts, rank, width // copies))


def solution(mesh):
    at = mesh.axis_names.index("expert")
    shape = mesh.devices.shape
    devices = mesh.devices.reshape(*shape[:at], shape[at] // 2, 2, *shape[at + 1 :])
    names = (*mesh.axis_names[:at], "chip", "core", *mesh.axis_names[at + 1 :])
    expert = ("chip", "core")
    return jax.shard_map(
        local,
        mesh=Mesh(devices, names),
        in_specs=(
            P("dp", expert, None),
            P("dp", expert, None),
            P("dp", expert, None),
            P("dp", expert, None, None),
            P(expert, None, None),
        ),
        out_specs=(P(expert, None, None), P(expert, None, "dp")),
        check_vma=False,
    )
```

```python
import math

import jax
import jax.numpy as jnp
from jax import lax
from jax.experimental import pallas as pl
from jax.experimental.pallas import tpu as pltpu
from jax.sharding import Mesh, PartitionSpec as P


F32 = jnp.float32
BF16 = jnp.bfloat16
HIGHEST = lax.Precision.HIGHEST
NN = (((1,), (0,)), ((), ()))
NT = (((1,), (1,)), ((), ()))
CP = 8
CAP = 6
STREAMS = 2


def params(limit_mib=48, **kw):
    return pltpu.CompilerParams(vmem_limit_bytes=limit_mib * 2**20, **kw)


def shape_of(shape, dtype):
    return jax.ShapeDtypeStruct(shape, dtype)


def in_hbm(shape, dtype):
    return pltpu.HBM(shape, dtype)


def from_hbm(value):
    return pltpu.with_memory_space_constraint(value, pltpu.HBM)


def place_rows(out_ref, turned, first, part_rows, base):
    done = 0
    while done < turned.shape[0]:
        chip, offset = divmod(first + done, part_rows)
        step = min(turned.shape[0] - done, part_rows - offset)
        out_ref[chip, base + offset : base + offset + step, :] = turned[done : done + step]
        done += step


def prepare_kernel(ids_ref, gates_ref, grads_ref, out_ref):
    ids = ids_ref[...].T
    gates = gates_ref[...].T
    chips, total, _ = out_ref.shape
    tokens, top = ids.shape
    width = grads_ref.shape[1]
    shape = (tokens, 256)
    lane = lax.broadcasted_iota(jnp.int32, shape, 1)
    rem = lane % 128
    expert = 16 * (rem // 8) + 8 * (lane // 128) + rem % 8
    hit = jnp.zeros(shape, F32)
    gate = jnp.zeros(shape, F32)
    for k in range(top):
        same = ids[:, k : k + 1] == expert
        hit = jnp.where(same, 1.0, hit)
        gate = jnp.where(same, gates[:, k : k + 1], gate)
    row = lax.broadcasted_iota(jnp.int32, (tokens, tokens), 0)
    col = lax.broadcasted_iota(jnp.int32, (tokens, tokens), 1)
    before = jnp.where(col < row, 1.0, 0.0).astype(BF16)
    pos = lax.dot_general(before, hit.astype(BF16), NN, preferred_element_type=F32)
    pos = jnp.where(hit > 0, pos, -1.0)
    token = lax.broadcasted_iota(jnp.int32, shape, 0).astype(F32)
    token_rows, gate_rows = [], []
    for c in range(CP):
        here = pos == c
        token_rows.append(jnp.max(jnp.where(here, token, -1.0), axis=0, keepdims=True))
        gate_rows.append(jnp.sum(jnp.where(here, gate, 0.0), axis=0, keepdims=True))
    table = jnp.concatenate(token_rows + gate_rows, axis=0).astype(BF16)
    table = jnp.concatenate([table[:, :128], table[:, 128:]], axis=0)
    codes_at = total - 4 * CP
    for j in range(chips):
        out_ref[j, codes_at:, :] = table
    copies = 4
    span = width // copies
    part = span // chips
    for p in range(copies):
        for n in range(span // 128):
            turned = grads_ref[:, p * span + n * 128 : p * span + (n + 1) * 128].T
            place_rows(out_ref, turned, n * 128, part, p * part)


def prepare(ids, gates, grads, chips):
    tokens, width = grads.shape
    return pl.pallas_call(
        prepare_kernel,
        out_shape=in_hbm((chips, width // chips + 4 * CP, tokens), BF16),
        compiler_params=params(),
        name="prepare",
    )(from_hbm(ids.T), from_hbm(gates.T), from_hbm(grads))


def turn_kernel(copy_ref, q_ref, out_ref):
    for n in range(q_ref.shape[1] // 128):
        out_ref[n * 128 : (n + 1) * 128, :] = q_ref[:, n * 128 : (n + 1) * 128].T


def turned_part(copy, q, copies):
    rows, width = q.shape
    steps = 2
    columns = width // copies
    return pl.pallas_call(
        turn_kernel,
        grid_spec=pltpu.PrefetchScalarGridSpec(
            num_scalar_prefetch=1,
            grid=(steps,),
            in_specs=[pl.BlockSpec((rows, columns // steps), lambda i, c: (0, c[0] * steps + i))],
            out_specs=pl.BlockSpec((columns // steps, rows), lambda i, c: (i, 0)),
        ),
        out_shape=in_hbm((columns, rows), BF16),
        compiler_params=params(),
        name="turned_part",
    )(copy, from_hbm(q))


def dispatch_kernel(core_ref, xt_ref, out_ref):
    core = core_ref[0]
    token = lax.broadcasted_iota(jnp.int32, (CP, 128), 1).astype(F32)
    group = 32
    width = out_ref.shape[2]
    start = pl.multiple_of(width + 2 * CP * core, 2 * CP)
    codes = []
    for i in range(2):
        table = xt_ref[i, pl.ds(start, 2 * CP), :].astype(F32)
        codes.append(table[:CP] + table[CP:])
    for g in range(128 // group):
        rows = []
        for i in range(2):
            parts = []
            for x in range(g * group, (g + 1) * group):
                u = codes[i][:, x : x + 1] - token
                parts.append(jnp.where((u > 0) & (u < 1), u, 0.0))
            picks = jnp.concatenate(parts, axis=0).astype(BF16)
            got = lax.dot_general(picks, xt_ref[i, :width], NT, preferred_element_type=F32)
            rows.append(got.reshape(group, CP, width))
        out_ref[g * group : (g + 1) * group] = jnp.concatenate(rows, axis=1).astype(BF16)


def dispatch(core, xt):
    chips, total, tokens = xt.shape
    width = total - 4 * CP

    def body(*refs):
        dispatch_kernel(*refs)

    return pl.pallas_call(
        body,
        grid_spec=pltpu.PrefetchScalarGridSpec(
            num_scalar_prefetch=1,
            grid=(chips // 2,),
            in_specs=[pl.BlockSpec((2, total, tokens), lambda i, _: (i, 0, 0))],
            out_specs=pl.BlockSpec((128, 2 * CP, width), lambda i, _: (0, i, 0)),
        ),
        out_shape=shape_of((128, chips * CP, width), BF16),
        compiler_params=params(),
        cost_estimate=pl.CostEstimate(
            flops=2 * 128 * CP * chips * tokens * width, bytes_accessed=128 * chips * CP * width * 2, transcendentals=0
        ),
    )(core, xt)


def mix_kernel(at_ref, own_ref, sib_ref, *rest):
    q_refs, (out_ref, q_ref, tmp_ref) = rest[:-3], rest[-3:]
    core, copy = at_ref[0], at_ref[1]
    copies = len(q_refs)
    lanes = out_ref.shape[4]
    owner = lax.broadcasted_iota(jnp.int32, (128, lanes), 1) // 32
    for n in range(out_ref.shape[0]):
        part = q_refs[0].shape[1]
        for shift, ref in enumerate(q_refs):
            start = pl.multiple_of(part * ((copy + shift) % copies), 16)
            q_ref[pl.ds(start, part), :] = ref[n]
        for half, ref in enumerate((own_ref, sib_ref)):
            _, experts, rows, width = ref.shape
            got = lax.dot_general(
                ref[n].reshape(experts * rows, width), q_ref[...], NN, preferred_element_type=F32
            )
            acc = got[:rows]
            for x in range(1, experts):
                acc = jnp.where(owner == x, got[x * rows : (x + 1) * rows], acc)
            tmp_ref[...] = acc
            place = core if half == 0 else 1 - core
            for c in range(CAP):
                out_ref[n, c, place] = tmp_ref[pl.ds(c, 16, stride=CP), :].astype(BF16)


def mix(at, own, sib, q_parts, stream):
    chips, part, lanes = q_parts[0].shape
    lanes = lanes // STREAMS
    _, experts, rows, width = own.shape
    experts = experts // STREAMS
    step = 2
    block = pl.BlockSpec((step, experts, rows, width), lambda i, _: (i, stream, 0, 0))
    q_block = pl.BlockSpec((step, part, lanes), lambda i, _: (i, 0, stream))
    return pl.pallas_call(
        mix_kernel,
        grid_spec=pltpu.PrefetchScalarGridSpec(
            num_scalar_prefetch=1,
            grid=(chips // step,),
            in_specs=[block, block] + [q_block] * len(q_parts),
            out_specs=pl.BlockSpec((step, CAP, 2, 16, lanes), lambda i, _: (i, 0, 0, 0, 0)),
            scratch_shapes=[pltpu.VMEM((width, lanes), BF16), pltpu.VMEM((rows, lanes), F32)],
        ),
        out_shape=in_hbm((chips, CAP, 2, 16, lanes), BF16),
        compiler_params=params(),
        cost_estimate=pl.CostEstimate(
            flops=4 * chips * experts * rows * width * 256,
            bytes_accessed=4 * chips * experts * rows * width,
            transcendentals=0,
        ),
    )(at, own, sib, *q_parts)


def factor_kernel(copy_ref, parts_ref, hidden_ref, *refs):
    out_refs, (tmp_ref, lhs_ref) = refs[:-2], refs[-2:]
    copies = len(out_refs)
    step = pl.program_id(0)
    here = hidden_ref.shape[0]

    @pl.when(step == 0)
    def _():
        for c in range(CAP):
            for k in range(2):
                total = parts_ref[0, c, k].astype(F32)
                for j in range(1, parts_ref.shape[0]):
                    total = total + parts_ref[j, c, k].astype(F32)
                tmp_ref[pl.ds(k * CAP + c, 16, stride=2 * CAP), :] = total
        lhs_ref[...] = tmp_ref[...].T.astype(BF16)

    for n in range(here):
        start = pl.multiple_of((step * here + n) * 32, 32)
        lhs = lhs_ref[pl.ds(start, 32), 0 : hidden_ref.shape[1]]
        value = lax.dot_general(lhs, hidden_ref[n], NN, preferred_element_type=F32).astype(BF16)
        ahead = (step * here + n - copy_ref[0] + copies) % copies
        for k, out_ref in enumerate(out_refs):

            @pl.when(ahead == k)
            def _():
                out_ref[...] = value


def first_factor(copy, parts, hidden, stream, copies):
    experts, slots, units = hidden.shape
    experts = experts // STREAMS
    lanes = parts.shape[4]
    step = 2
    first = stream * experts // step
    return pl.pallas_call(
        factor_kernel,
        grid_spec=pltpu.PrefetchScalarGridSpec(
            num_scalar_prefetch=1,
            grid=(experts // step,),
            in_specs=[
                pl.BlockSpec(parts.shape, lambda i, _: (0, 0, 0, 0, 0)),
                pl.BlockSpec((step, slots, units), lambda i, _: (first + i, 0, 0)),
            ],
            out_specs=[pl.BlockSpec((32, units), lambda i, _: (0, 0))] * copies,
            scratch_shapes=[pltpu.VMEM((256, lanes), F32), pltpu.VMEM((lanes, 256), BF16)],
        ),
        out_shape=[shape_of((32, units), BF16)] * copies,
        compiler_params=params(),
        cost_estimate=pl.CostEstimate(
            flops=2 * experts * slots * units * 256, bytes_accessed=2 * experts * slots * units, transcendentals=0
        ),
    )(copy, parts, hidden)


def ortho_kernel(*refs):
    parts_refs, out_ref = refs[:-1], refs[-1]
    row = lax.broadcasted_iota(jnp.int32, (32, 32), 0)
    col = lax.broadcasted_iota(jnp.int32, (32, 32), 1)
    value = parts_refs[0][...].astype(F32)
    for ref in parts_refs[1:]:
        value = value + ref[...].astype(F32)
    gram = lax.dot_general(value, value, NT, precision=HIGHEST, preferred_element_type=F32)
    a = jnp.concatenate([gram, jnp.where(row == col, 1.0, 0.0)], axis=1)
    index = lax.broadcasted_iota(jnp.int32, (32, 64), 0)
    for k in range(32):
        inv = lax.rsqrt(a[k : k + 1, k : k + 1])
        pivot = a[k : k + 1, :] * inv
        lower = a[:, k : k + 1] * inv
        below = a - lower * pivot
        a = jnp.where(index > k, below, jnp.where(index == k, pivot, a))
    out_ref[...] = lax.dot_general(
        a[:, 32:], value, NN, precision=HIGHEST, preferred_element_type=F32
    ).astype(BF16)


def ortho_of(parts):
    rank, units = parts[0].shape
    return pl.pallas_call(
        ortho_kernel,
        out_shape=shape_of((rank, units), BF16),
        compiler_params=params(),
        cost_estimate=pl.CostEstimate(flops=5_000_000_000, bytes_accessed=4 * rank * units * 2, transcendentals=0),
    )(*parts)


def project_kernel(copy_ref, *refs, copies):
    part_refs, hidden_ref = refs[:copies], refs[copies]
    basis_ref, out_ref, ortho_ref, rows_ref = refs[-4:]
    step = pl.program_id(0)
    here, slots, units = hidden_ref.shape

    @pl.when(step == 0)
    def _():
        for k, ref in enumerate(part_refs):
            place = pl.multiple_of(32 * ((copy_ref[0] - k + copies) % copies), 32)
            ortho_ref[pl.ds(place, 32), :] = ref[...]

    start = pl.multiple_of(step * here * 32, 32)
    basis = ortho_ref[pl.ds(start, here * 32), :].astype(F32) * math.sqrt(units)
    basis_ref[...] = basis.reshape(here, 32, units)
    got = lax.dot_general(
        hidden_ref[...].reshape(here * slots, units), ortho_ref[...], NT, preferred_element_type=F32
    )
    owner = lax.broadcasted_iota(jnp.int32, (slots, ortho_ref.shape[0]), 1) // 32
    for n in range(here):
        value = got[n * slots : (n + 1) * slots]
        kept = rows_ref[...]
        rows_ref[...] = jnp.where(owner == step * here + n, value, kept)

    @pl.when(step == pl.num_programs(0) - 1)
    def _():
        for c in range(CAP):
            for k in range(2):
                value = rows_ref[pl.ds(k * CAP + c, 16, stride=2 * CAP), :].astype(BF16)
                for j in range(out_ref.shape[0]):
                    out_ref[j, c, k] = value


def project(copy, parts, hidden, stream, basis, chips):
    every, slots, units = hidden.shape
    experts = every // STREAMS
    copies = len(parts)
    lanes = experts * 32
    step = 2
    first = stream * experts // step
    given = [] if basis is None else [basis]

    def body(*refs):
        project_kernel(*refs, copies=copies)

    return pl.pallas_call(
        body,
        grid_spec=pltpu.PrefetchScalarGridSpec(
            num_scalar_prefetch=1,
            grid=(experts // step,),
            in_specs=[pl.BlockSpec((32, units), lambda i, _: (0, 0))] * copies
            + [pl.BlockSpec((step, slots, units), lambda i, _: (first + i, 0, 0))]
            + [pl.BlockSpec(memory_space=pl.ANY)] * len(given),
            out_specs=[
                pl.BlockSpec((step, 32, units), lambda i, _: (first + i, 0, 0)),
                pl.BlockSpec((chips, CAP, 2, 16, lanes), lambda i, _: (0, 0, 0, 0, 0)),
            ],
            scratch_shapes=[pltpu.VMEM((lanes, units), BF16), pltpu.VMEM((slots, lanes), F32)],
        ),
        out_shape=[
            shape_of((every, 32, units), F32),
            in_hbm((chips, CAP, 2, 16, lanes), BF16),
        ],
        input_output_aliases={copies + 2: 0} if given else {},
        compiler_params=params(),
        cost_estimate=pl.CostEstimate(
            flops=2 * experts * slots * units * 256, bytes_accessed=2 * experts * slots * units, transcendentals=0
        ),
    )(copy, *parts, hidden, *given)


def terms_kernel(core_ref, own_ref, sib_ref, proj_ref, out_ref, rows_ref, sum_ref):
    core = core_ref[0]
    count, experts, _, width = own_ref.shape
    part = width // 4

    @pl.when(pl.program_id(0) == 0)
    def _():
        rows_ref[...] = jnp.zeros_like(rows_ref)
        sum_ref[...] = jnp.zeros_like(sum_ref)

    for n in range(count):
        for half in range(2):
            place = core if half == 0 else 1 - core
            for c in range(CAP):
                rows_ref[pl.ds(half * 128 + c, 16, stride=CP), :] = proj_ref[n, c, place].astype(F32)
        turned = rows_ref[...].T.astype(BF16)
        for x in range(experts):
            both = jnp.concatenate([own_ref[n, x], sib_ref[n, x]], axis=0)
            got = lax.dot_general(turned[x * 32 : (x + 1) * 32], both, NN, preferred_element_type=F32)
            sum_ref[x * 32 : (x + 1) * 32, 0:width] = got
        for i in range(4):
            tall = min(width - i * 128, 128)
            back = sum_ref[:, i * 128 : (i + 1) * 128].T[:tall].astype(BF16)
            done = 0
            while done < tall:
                p, offset = divmod(i * 128 + done, part)
                step = min(tall - done, part - offset)
                out_ref[p, n, offset : offset + step, :] = back[done : done + step]
                done += step


def second_terms(core, own, sib, proj, stream):
    chips, _, _, _, lanes = proj.shape
    _, experts, rows, width = own.shape
    experts = experts // STREAMS
    step = 2
    block = pl.BlockSpec((step, experts, rows, width), lambda i, _: (i, stream, 0, 0))
    return pl.pallas_call(
        terms_kernel,
        grid_spec=pltpu.PrefetchScalarGridSpec(
            num_scalar_prefetch=1,
            grid=(chips // step,),
            in_specs=[block, block, pl.BlockSpec((step, CAP, 2, 16, lanes), lambda i, _: (i, 0, 0, 0, 0))],
            out_specs=pl.BlockSpec((4, step, width // 4, lanes), lambda i, _: (0, i, 0, 0)),
            scratch_shapes=[pltpu.VMEM((256, lanes), F32), pltpu.VMEM((lanes, 512), F32)],
        ),
        out_shape=in_hbm((4, chips, width // 4, lanes), BF16),
        compiler_params=params(),
        cost_estimate=pl.CostEstimate(
            flops=4 * chips * experts * rows * width * 256,
            bytes_accessed=4 * chips * experts * rows * width,
            transcendentals=0,
        ),
    )(core, own, sib, proj)


def gather_kernel(parts_ref, *refs):
    out_ref = refs[-1]
    total = parts_ref[0].astype(F32)
    for p in range(1, parts_ref.shape[0]):
        total = total + parts_ref[p].astype(F32)
    out_ref[...] = total.T


def owned_columns(parts, stream, sums):
    copies, columns, rows = parts.shape
    given = [] if sums is None else [sums]
    wide = 896
    return pl.pallas_call(
        gather_kernel,
        grid=(columns // wide,),
        in_specs=[pl.BlockSpec((copies, wide, rows), lambda i: (0, i, 0))]
        + [pl.BlockSpec(memory_space=pl.ANY)] * len(given),
        out_specs=pl.BlockSpec((rows, wide), lambda i: (stream, i)),
        out_shape=shape_of((rows * STREAMS, columns), F32),
        input_output_aliases={1: 0} if given else {},
        compiler_params=params(),
    )(parts, *given)


def exchange(values, axes):
    return lax.all_to_all(values, axes, split_axis=0, concat_axis=0, tiled=True)


def shift(value, step, copies):
    return lax.ppermute(value, "dp", [(i, (i + step) % copies) for i in range(copies)])


def around(part, copies):
    half = part.shape[0] // 2
    before = shift(part, 1, copies)
    after = shift(part, copies - 1, copies)
    far_low = shift(before[:half], 1, copies)
    far_high = shift(after[half:], copies - 1, copies)
    return [part, after, jnp.concatenate([far_low, far_high], axis=0), before]


def whole(out_grads, expert_ids, gate_probs, hidden_acts, q_previous):
    chips = lax.axis_size("chip")
    copies = lax.axis_size("dp")
    core = lax.axis_index("core").astype(jnp.int32).reshape(1)
    copy = lax.axis_index("dp").astype(jnp.int32).reshape(1)
    at = jnp.concatenate([core, copy])
    hidden = hidden_acts[0]
    experts, rank, width = q_previous.shape
    here = experts // STREAMS

    q_part = turned_part(copy, q_previous.reshape(experts * rank, width), copies)
    q_part = exchange(q_part.reshape(chips, -1, experts * rank), "chip")
    own_t = prepare(expert_ids[0], gate_probs[0], out_grads[0], chips)
    q_part, own_t = lax.optimization_barrier((q_part, own_t))
    q_parts = around(q_part, copies)
    own_t = exchange(own_t, "chip")
    sib_t = lax.ppermute(own_t, "core", [(0, 1), (1, 0)])
    own = dispatch(core, own_t)
    sib = dispatch(core, sib_t)
    own = own.reshape(chips, experts, *own.shape[1:])
    sib = sib.reshape(chips, experts, *sib.shape[1:])

    basis, sums = None, None
    for s in range(STREAMS):
        mixed = exchange(mix(at, own, sib, q_parts, s), "chip")
        factor = first_factor(copy, mixed, hidden, s, copies)
        factor = [factor[0]] + [shift(factor[k], k, copies) for k in range(1, copies)]
        ortho = ortho_of(factor)
        ortho = [ortho] + [shift(ortho, k, copies) for k in range(1, copies)]
        basis, proj = project(copy, ortho, hidden, s, basis, chips)
        terms = second_terms(core, own, sib, exchange(proj, "chip"), s)
        terms = exchange(terms.reshape(copies * chips, -1, here * rank), ("dp", "chip"))
        sums = owned_columns(terms.reshape(copies, width // copies, here * rank), s, sums)
    return (basis, sums.reshape(experts, rank, width // copies))


def solution(mesh):
    at = mesh.axis_names.index("expert")
    shape = mesh.devices.shape
    devices = mesh.devices.reshape(*shape[:at], shape[at] // 2, 2, *shape[at + 1 :])
    names = (*mesh.axis_names[:at], "chip", "core", *mesh.axis_names[at + 1 :])
    expert = ("chip", "core")
    return jax.shard_map(
        whole,
        mesh=Mesh(devices, names),
        in_specs=(
            P("dp", expert, None),
            P("dp", expert, None),
            P("dp", expert, None),
            P("dp", expert, None, None),
            P(expert, None, None),
        ),
        out_specs=(P(expert, None, None), P(expert, None, "dp")),
        check_vma=False,
    )
```

```python
import math

import jax
import jax.numpy as jnp
from jax import lax
from jax.experimental import pallas as pl
from jax.experimental.pallas import tpu as pltpu
from jax.sharding import Mesh, PartitionSpec as P


F32 = jnp.float32
BF16 = jnp.bfloat16
HIGHEST = lax.Precision.HIGHEST
NN = (((1,), (0,)), ((), ()))
NT = (((1,), (1,)), ((), ()))
CP = 8
CAP = 6
STREAMS = 2
STEP = 2
AHEAD = 3


def params(limit_mib=48, **kw):
    return pltpu.CompilerParams(vmem_limit_bytes=limit_mib * 2**20, **kw)


def shape_of(shape, dtype):
    return jax.ShapeDtypeStruct(shape, dtype)


def in_hbm(shape, dtype):
    return pltpu.HBM(shape, dtype)


def from_hbm(value):
    return pltpu.with_memory_space_constraint(value, pltpu.HBM)


def place_rows(out_ref, turned, first, part_rows, base):
    done = 0
    while done < turned.shape[0]:
        chip, offset = divmod(first + done, part_rows)
        step = min(turned.shape[0] - done, part_rows - offset)
        out_ref[chip, base + offset : base + offset + step, :] = turned[done : done + step]
        done += step


def prepare_kernel(ids_ref, gates_ref, grads_ref, out_ref):
    ids = ids_ref[...].T
    gates = gates_ref[...].T
    chips, total, _ = out_ref.shape
    tokens, top = ids.shape
    width = grads_ref.shape[1]
    shape = (tokens, 256)
    lane = lax.broadcasted_iota(jnp.int32, shape, 1)
    rem = lane % 128
    expert = 16 * (rem // 8) + 8 * (lane // 128) + rem % 8
    hit = jnp.zeros(shape, F32)
    gate = jnp.zeros(shape, F32)
    for k in range(top):
        same = ids[:, k : k + 1] == expert
        hit = jnp.where(same, 1.0, hit)
        gate = jnp.where(same, gates[:, k : k + 1], gate)
    row = lax.broadcasted_iota(jnp.int32, (tokens, tokens), 0)
    col = lax.broadcasted_iota(jnp.int32, (tokens, tokens), 1)
    before = jnp.where(col < row, 1.0, 0.0).astype(BF16)
    pos = lax.dot_general(before, hit.astype(BF16), NN, preferred_element_type=F32)
    pos = jnp.where(hit > 0, pos, -1.0)
    token = lax.broadcasted_iota(jnp.int32, shape, 0).astype(F32)
    token_rows, gate_rows = [], []
    for c in range(CP):
        here = pos == c
        token_rows.append(jnp.max(jnp.where(here, token, -1.0), axis=0, keepdims=True))
        gate_rows.append(jnp.sum(jnp.where(here, gate, 0.0), axis=0, keepdims=True))
    table = jnp.concatenate(token_rows + gate_rows, axis=0).astype(BF16)
    table = jnp.concatenate([table[:, :128], table[:, 128:]], axis=0)
    codes_at = total - 4 * CP
    for j in range(chips):
        out_ref[j, codes_at:, :] = table
    copies = 4
    span = width // copies
    part = span // chips
    for p in range(copies):
        for n in range(span // 128):
            turned = grads_ref[:, p * span + n * 128 : p * span + (n + 1) * 128].T
            place_rows(out_ref, turned, n * 128, part, p * part)


def prepare(ids, gates, grads, chips):
    tokens, width = grads.shape
    return pl.pallas_call(
        prepare_kernel,
        out_shape=in_hbm((chips, width // chips + 4 * CP, tokens), BF16),
        compiler_params=params(),
        name="prepare",
    )(from_hbm(ids.T), from_hbm(gates.T), from_hbm(grads))


def turn_kernel(copy_ref, q_ref, out_ref):
    for n in range(q_ref.shape[1] // 128):
        out_ref[n * 128 : (n + 1) * 128, :] = q_ref[:, n * 128 : (n + 1) * 128].T


def turned_part(copy, q, copies):
    rows, width = q.shape
    steps = 2
    columns = width // copies
    return pl.pallas_call(
        turn_kernel,
        grid_spec=pltpu.PrefetchScalarGridSpec(
            num_scalar_prefetch=1,
            grid=(steps,),
            in_specs=[pl.BlockSpec((rows, columns // steps), lambda i, c: (0, c[0] * steps + i))],
            out_specs=pl.BlockSpec((columns // steps, rows), lambda i, c: (i, 0)),
        ),
        out_shape=in_hbm((columns, rows), BF16),
        compiler_params=params(),
        name="turned_part",
    )(copy, from_hbm(q))


def dispatch_kernel(core_ref, xt_ref, out_ref):
    core = core_ref[0]
    token = lax.broadcasted_iota(jnp.int32, (CP, 128), 1).astype(F32)
    group = 32
    width = out_ref.shape[2]
    start = pl.multiple_of(width + 2 * CP * core, 2 * CP)
    codes = []
    for i in range(2):
        table = xt_ref[i, pl.ds(start, 2 * CP), :].astype(F32)
        codes.append(table[:CP] + table[CP:])
    for g in range(128 // group):
        rows = []
        for i in range(2):
            parts = []
            for x in range(g * group, (g + 1) * group):
                u = codes[i][:, x : x + 1] - token
                parts.append(jnp.where((u > 0) & (u < 1), u, 0.0))
            picks = jnp.concatenate(parts, axis=0).astype(BF16)
            got = lax.dot_general(picks, xt_ref[i, :width], NT, preferred_element_type=F32)
            rows.append(got.reshape(group, CP, width))
        out_ref[g * group : (g + 1) * group] = jnp.concatenate(rows, axis=1).astype(BF16)


def dispatch(core, xt):
    chips, total, tokens = xt.shape
    width = total - 4 * CP

    def body(*refs):
        dispatch_kernel(*refs)

    return pl.pallas_call(
        body,
        grid_spec=pltpu.PrefetchScalarGridSpec(
            num_scalar_prefetch=1,
            grid=(chips // 2,),
            in_specs=[pl.BlockSpec((2, total, tokens), lambda i, _: (i, 0, 0))],
            out_specs=pl.BlockSpec((128, 2 * CP, width), lambda i, _: (0, i, 0)),
        ),
        out_shape=shape_of((128, chips * CP, width), BF16),
        compiler_params=params(),
        cost_estimate=pl.CostEstimate(
            flops=2 * 128 * CP * chips * tokens * width, bytes_accessed=128 * chips * CP * width * 2, transcendentals=0
        ),
    )(core, xt)


def arrived_rows(sources, rows_ref, sems, stream):
    step = pl.program_id(0)
    _, every, count, experts, _, _ = rows_ref.shape

    def copy(half, i):
        return pltpu.make_async_copy(
            sources[half].at[pl.ds(i * count, count), stream * experts : (stream + 1) * experts],
            rows_ref.at[half, i],
            sems.at[half, i],
        )

    @pl.when(step == 0)
    def _():
        for i in range(AHEAD):
            for half in range(2):
                copy(half, i).start()

    @pl.when(step + AHEAD < every)
    def _():
        for half in range(2):
            copy(half, step + AHEAD).start()

    for half in range(2):
        copy(half, step).wait()
    return rows_ref.at[0, step], rows_ref.at[1, step]


def mix_kernel(at_ref, own_ref, sib_ref, *rest, stream):
    q_refs, (out_ref, q_ref, tmp_ref, rows_ref, sems) = rest[:-5], rest[-5:]
    own_ref, sib_ref = arrived_rows((own_ref, sib_ref), rows_ref, sems, stream)
    core, copy = at_ref[0], at_ref[1]
    copies = len(q_refs)
    lanes = out_ref.shape[4]
    owner = lax.broadcasted_iota(jnp.int32, (128, lanes), 1) // 32
    for n in range(out_ref.shape[0]):
        part = q_refs[0].shape[1]
        for shift, ref in enumerate(q_refs):
            start = pl.multiple_of(part * ((copy + shift) % copies), 16)
            q_ref[pl.ds(start, part), :] = ref[n]
        for half, ref in enumerate((own_ref, sib_ref)):
            _, experts, rows, width = ref.shape
            got = lax.dot_general(
                ref[n].reshape(experts * rows, width), q_ref[...], NN, preferred_element_type=F32
            )
            acc = got[:rows]
            for x in range(1, experts):
                acc = jnp.where(owner == x, got[x * rows : (x + 1) * rows], acc)
            tmp_ref[...] = acc
            place = core if half == 0 else 1 - core
            for c in range(CAP):
                out_ref[n, c, place] = tmp_ref[pl.ds(c, 16, stride=CP), :].astype(BF16)


def mix(at, own, sib, q_parts, stream):
    chips, part, lanes = q_parts[0].shape
    lanes = lanes // STREAMS
    _, experts, rows, width = own.shape
    experts = experts // STREAMS
    step = STEP
    block = pl.BlockSpec(memory_space=pl.ANY)

    def body(*refs):
        mix_kernel(*refs, stream=stream)

    q_block = pl.BlockSpec((step, part, lanes), lambda i, _: (i, 0, stream))
    return pl.pallas_call(
        body,
        grid_spec=pltpu.PrefetchScalarGridSpec(
            num_scalar_prefetch=1,
            grid=(chips // step,),
            in_specs=[block, block] + [q_block] * len(q_parts),
            out_specs=pl.BlockSpec((step, CAP, 2, 16, lanes), lambda i, _: (i, 0, 0, 0, 0)),
            scratch_shapes=[
                pltpu.VMEM((width, lanes), BF16),
                pltpu.VMEM((rows, lanes), F32),
                pltpu.VMEM((2, chips // step, step, experts, rows, width), BF16),
                pltpu.SemaphoreType.DMA((2, chips // step)),
            ],
        ),
        out_shape=in_hbm((chips, CAP, 2, 16, lanes), BF16),
        compiler_params=params(),
        cost_estimate=pl.CostEstimate(
            flops=4 * chips * experts * rows * width * 256,
            bytes_accessed=4 * chips * experts * rows * width,
            transcendentals=0,
        ),
    )(at, own, sib, *q_parts)


def factor_kernel(copy_ref, parts_ref, hidden_ref, *refs):
    out_refs, (tmp_ref, lhs_ref) = refs[:-2], refs[-2:]
    copies = len(out_refs)
    step = pl.program_id(0)
    here = hidden_ref.shape[0]

    @pl.when(step == 0)
    def _():
        for c in range(CAP):
            for k in range(2):
                total = parts_ref[0, c, k].astype(F32)
                for j in range(1, parts_ref.shape[0]):
                    total = total + parts_ref[j, c, k].astype(F32)
                tmp_ref[pl.ds(k * CAP + c, 16, stride=2 * CAP), :] = total
        lhs_ref[...] = tmp_ref[...].T.astype(BF16)

    for n in range(here):
        start = pl.multiple_of((step * here + n) * 32, 32)
        lhs = lhs_ref[pl.ds(start, 32), 0 : hidden_ref.shape[1]]
        value = lax.dot_general(lhs, hidden_ref[n], NN, preferred_element_type=F32).astype(BF16)
        ahead = (step * here + n - copy_ref[0] + copies) % copies
        for k, out_ref in enumerate(out_refs):

            @pl.when(ahead == k)
            def _():
                out_ref[...] = value


def first_factor(copy, parts, hidden, stream, copies):
    experts, slots, units = hidden.shape
    experts = experts // STREAMS
    lanes = parts.shape[4]
    step = 2
    first = stream * experts // step
    return pl.pallas_call(
        factor_kernel,
        grid_spec=pltpu.PrefetchScalarGridSpec(
            num_scalar_prefetch=1,
            grid=(experts // step,),
            in_specs=[
                pl.BlockSpec(parts.shape, lambda i, _: (0, 0, 0, 0, 0)),
                pl.BlockSpec((step, slots, units), lambda i, _: (first + i, 0, 0)),
            ],
            out_specs=[pl.BlockSpec((32, units), lambda i, _: (0, 0))] * copies,
            scratch_shapes=[pltpu.VMEM((256, lanes), F32), pltpu.VMEM((lanes, 256), BF16)],
        ),
        out_shape=[shape_of((32, units), BF16)] * copies,
        compiler_params=params(),
        cost_estimate=pl.CostEstimate(
            flops=2 * experts * slots * units * 256, bytes_accessed=2 * experts * slots * units, transcendentals=0
        ),
    )(copy, parts, hidden)


def ortho_kernel(*refs):
    parts_refs, out_ref = refs[:-1], refs[-1]
    row = lax.broadcasted_iota(jnp.int32, (32, 32), 0)
    col = lax.broadcasted_iota(jnp.int32, (32, 32), 1)
    value = parts_refs[0][...].astype(F32)
    for ref in parts_refs[1:]:
        value = value + ref[...].astype(F32)
    gram = lax.dot_general(value, value, NT, precision=HIGHEST, preferred_element_type=F32)
    a = jnp.concatenate([gram, jnp.where(row == col, 1.0, 0.0)], axis=1)
    index = lax.broadcasted_iota(jnp.int32, (32, 64), 0)
    for k in range(32):
        inv = lax.rsqrt(a[k : k + 1, k : k + 1])
        pivot = a[k : k + 1, :] * inv
        lower = a[:, k : k + 1] * inv
        below = a - lower * pivot
        a = jnp.where(index > k, below, jnp.where(index == k, pivot, a))
    out_ref[...] = lax.dot_general(
        a[:, 32:], value, NN, precision=HIGHEST, preferred_element_type=F32
    ).astype(BF16)


def ortho_of(parts):
    rank, units = parts[0].shape
    return pl.pallas_call(
        ortho_kernel,
        out_shape=shape_of((rank, units), BF16),
        compiler_params=params(),
        cost_estimate=pl.CostEstimate(flops=5_000_000_000, bytes_accessed=4 * rank * units * 2, transcendentals=0),
    )(*parts)


def project_kernel(copy_ref, *refs, copies):
    part_refs, hidden_ref = refs[:copies], refs[copies]
    basis_ref, out_ref, ortho_ref, rows_ref = refs[-4:]
    step = pl.program_id(0)
    here, slots, units = hidden_ref.shape

    @pl.when(step == 0)
    def _():
        for k, ref in enumerate(part_refs):
            place = pl.multiple_of(32 * ((copy_ref[0] - k + copies) % copies), 32)
            ortho_ref[pl.ds(place, 32), :] = ref[...]

    start = pl.multiple_of(step * here * 32, 32)
    basis = ortho_ref[pl.ds(start, here * 32), :].astype(F32) * math.sqrt(units)
    basis_ref[...] = basis.reshape(here, 32, units)
    got = lax.dot_general(
        hidden_ref[...].reshape(here * slots, units), ortho_ref[...], NT, preferred_element_type=F32
    )
    owner = lax.broadcasted_iota(jnp.int32, (slots, ortho_ref.shape[0]), 1) // 32
    for n in range(here):
        value = got[n * slots : (n + 1) * slots]
        kept = rows_ref[...]
        rows_ref[...] = jnp.where(owner == step * here + n, value, kept)

    @pl.when(step == pl.num_programs(0) - 1)
    def _():
        for c in range(CAP):
            for k in range(2):
                value = rows_ref[pl.ds(k * CAP + c, 16, stride=2 * CAP), :].astype(BF16)
                for j in range(out_ref.shape[0]):
                    out_ref[j, c, k] = value


def project(copy, parts, hidden, stream, basis, chips):
    every, slots, units = hidden.shape
    experts = every // STREAMS
    copies = len(parts)
    lanes = experts * 32
    step = 2
    first = stream * experts // step
    given = [] if basis is None else [basis]

    def body(*refs):
        project_kernel(*refs, copies=copies)

    return pl.pallas_call(
        body,
        grid_spec=pltpu.PrefetchScalarGridSpec(
            num_scalar_prefetch=1,
            grid=(experts // step,),
            in_specs=[pl.BlockSpec((32, units), lambda i, _: (0, 0))] * copies
            + [pl.BlockSpec((step, slots, units), lambda i, _: (first + i, 0, 0))]
            + [pl.BlockSpec(memory_space=pl.ANY)] * len(given),
            out_specs=[
                pl.BlockSpec((step, 32, units), lambda i, _: (first + i, 0, 0)),
                pl.BlockSpec((chips, CAP, 2, 16, lanes), lambda i, _: (0, 0, 0, 0, 0)),
            ],
            scratch_shapes=[pltpu.VMEM((lanes, units), BF16), pltpu.VMEM((slots, lanes), F32)],
        ),
        out_shape=[
            shape_of((every, 32, units), F32),
            in_hbm((chips, CAP, 2, 16, lanes), BF16),
        ],
        input_output_aliases={copies + 2: 0} if given else {},
        compiler_params=params(),
        cost_estimate=pl.CostEstimate(
            flops=2 * experts * slots * units * 256, bytes_accessed=2 * experts * slots * units, transcendentals=0
        ),
    )(copy, *parts, hidden, *given)


def terms_kernel(core_ref, own_ref, sib_ref, proj_ref, out_ref, rows_ref, sum_ref, held_ref, sems, *, stream):
    core = core_ref[0]
    own_ref, sib_ref = arrived_rows((own_ref, sib_ref), held_ref, sems, stream)
    count, experts, _, width = own_ref.shape
    part = width // 4

    @pl.when(pl.program_id(0) == 0)
    def _():
        rows_ref[...] = jnp.zeros_like(rows_ref)
        sum_ref[...] = jnp.zeros_like(sum_ref)

    for n in range(count):
        for half in range(2):
            place = core if half == 0 else 1 - core
            for c in range(CAP):
                rows_ref[pl.ds(half * 128 + c, 16, stride=CP), :] = proj_ref[n, c, place].astype(F32)
        turned = rows_ref[...].T.astype(BF16)
        for x in range(experts):
            both = jnp.concatenate([own_ref[n, x], sib_ref[n, x]], axis=0)
            got = lax.dot_general(turned[x * 32 : (x + 1) * 32], both, NN, preferred_element_type=F32)
            sum_ref[x * 32 : (x + 1) * 32, 0:width] = got
        for i in range(4):
            tall = min(width - i * 128, 128)
            back = sum_ref[:, i * 128 : (i + 1) * 128].T[:tall].astype(BF16)
            done = 0
            while done < tall:
                p, offset = divmod(i * 128 + done, part)
                step = min(tall - done, part - offset)
                out_ref[p, n, offset : offset + step, :] = back[done : done + step]
                done += step


def second_terms(core, own, sib, proj, stream):
    chips, _, _, _, lanes = proj.shape
    _, experts, rows, width = own.shape
    experts = experts // STREAMS
    step = STEP
    block = pl.BlockSpec(memory_space=pl.ANY)

    def body(*refs):
        terms_kernel(*refs, stream=stream)

    return pl.pallas_call(
        body,
        grid_spec=pltpu.PrefetchScalarGridSpec(
            num_scalar_prefetch=1,
            grid=(chips // step,),
            in_specs=[block, block, pl.BlockSpec((step, CAP, 2, 16, lanes), lambda i, _: (i, 0, 0, 0, 0))],
            out_specs=pl.BlockSpec((4, step, width // 4, lanes), lambda i, _: (0, i, 0, 0)),
            scratch_shapes=[
                pltpu.VMEM((256, lanes), F32),
                pltpu.VMEM((lanes, 512), F32),
                pltpu.VMEM((2, chips // step, step, experts, rows, width), BF16),
                pltpu.SemaphoreType.DMA((2, chips // step)),
            ],
        ),
        out_shape=in_hbm((4, chips, width // 4, lanes), BF16),
        compiler_params=params(),
        cost_estimate=pl.CostEstimate(
            flops=4 * chips * experts * rows * width * 256,
            bytes_accessed=4 * chips * experts * rows * width,
            transcendentals=0,
        ),
    )(core, own, sib, proj)


def gather_kernel(parts_ref, *refs):
    out_ref = refs[-1]
    total = parts_ref[0].astype(F32)
    for p in range(1, parts_ref.shape[0]):
        total = total + parts_ref[p].astype(F32)
    out_ref[...] = total.T


def owned_columns(parts, stream, sums):
    copies, columns, rows = parts.shape
    given = [] if sums is None else [sums]
    wide = 896
    return pl.pallas_call(
        gather_kernel,
        grid=(columns // wide,),
        in_specs=[pl.BlockSpec((copies, wide, rows), lambda i: (0, i, 0))]
        + [pl.BlockSpec(memory_space=pl.ANY)] * len(given),
        out_specs=pl.BlockSpec((rows, wide), lambda i: (stream, i)),
        out_shape=shape_of((rows * STREAMS, columns), F32),
        input_output_aliases={1: 0} if given else {},
        compiler_params=params(),
    )(parts, *given)


def exchange(values, axes):
    return lax.all_to_all(values, axes, split_axis=0, concat_axis=0, tiled=True)


def shift(value, step, copies):
    return lax.ppermute(value, "dp", [(i, (i + step) % copies) for i in range(copies)])


def around(part, copies):
    half = part.shape[0] // 2
    before = shift(part, 1, copies)
    after = shift(part, copies - 1, copies)
    far_low = shift(before[:half], 1, copies)
    far_high = shift(after[half:], copies - 1, copies)
    return [part, after, jnp.concatenate([far_low, far_high], axis=0), before]


def whole(out_grads, expert_ids, gate_probs, hidden_acts, q_previous):
    chips = lax.axis_size("chip")
    copies = lax.axis_size("dp")
    core = lax.axis_index("core").astype(jnp.int32).reshape(1)
    copy = lax.axis_index("dp").astype(jnp.int32).reshape(1)
    at = jnp.concatenate([core, copy])
    hidden = hidden_acts[0]
    experts, rank, width = q_previous.shape
    here = experts // STREAMS

    q_part = turned_part(copy, q_previous.reshape(experts * rank, width), copies)
    q_part = exchange(q_part.reshape(chips, -1, experts * rank), "chip")
    own_t = prepare(expert_ids[0], gate_probs[0], out_grads[0], chips)
    q_part, own_t = lax.optimization_barrier((q_part, own_t))
    q_parts = around(q_part, copies)
    own_t = exchange(own_t, "chip")
    sib_t = lax.ppermute(own_t, "core", [(0, 1), (1, 0)])
    own = dispatch(core, own_t)
    sib = dispatch(core, sib_t)
    own = own.reshape(chips, experts, *own.shape[1:])
    sib = sib.reshape(chips, experts, *sib.shape[1:])

    basis, sums = None, None
    for s in range(STREAMS):
        mixed = exchange(mix(at, own, sib, q_parts, s), "chip")
        factor = first_factor(copy, mixed, hidden, s, copies)
        factor = [factor[0]] + [shift(factor[k], k, copies) for k in range(1, copies)]
        ortho = ortho_of(factor)
        ortho = [ortho] + [shift(ortho, k, copies) for k in range(1, copies)]
        basis, proj = project(copy, ortho, hidden, s, basis, chips)
        terms = second_terms(core, own, sib, exchange(proj, "chip"), s)
        terms = exchange(terms.reshape(copies * chips, -1, here * rank), ("dp", "chip"))
        sums = owned_columns(terms.reshape(copies, width // copies, here * rank), s, sums)
    return (basis, sums.reshape(experts, rank, width // copies))


def solution(mesh):
    at = mesh.axis_names.index("expert")
    shape = mesh.devices.shape
    devices = mesh.devices.reshape(*shape[:at], shape[at] // 2, 2, *shape[at + 1 :])
    names = (*mesh.axis_names[:at], "chip", "core", *mesh.axis_names[at + 1 :])
    expert = ("chip", "core")
    return jax.shard_map(
        whole,
        mesh=Mesh(devices, names),
        in_specs=(
            P("dp", expert, None),
            P("dp", expert, None),
            P("dp", expert, None),
            P("dp", expert, None, None),
            P(expert, None, None),
        ),
        out_specs=(P(expert, None, None), P(expert, None, "dp")),
        check_vma=False,
    )
```

```python
import math

import jax
import jax.numpy as jnp
from jax import lax
from jax.experimental import pallas as pl
from jax.experimental.pallas import tpu as pltpu
from jax.sharding import Mesh, PartitionSpec as P


F32 = jnp.float32
BF16 = jnp.bfloat16
HIGHEST = lax.Precision.HIGHEST
NN = (((1,), (0,)), ((), ()))
NT = (((1,), (1,)), ((), ()))
CP = 8
CAP = 6
STREAMS = 2
STEP = 2
AHEAD = 3


def params(limit_mib=48, **kw):
    return pltpu.CompilerParams(vmem_limit_bytes=limit_mib * 2**20, **kw)


def shape_of(shape, dtype):
    return jax.ShapeDtypeStruct(shape, dtype)


def in_hbm(shape, dtype):
    return pltpu.HBM(shape, dtype)


def from_hbm(value):
    return pltpu.with_memory_space_constraint(value, pltpu.HBM)


def place_rows(out_ref, turned, first, part_rows, base):
    done = 0
    while done < turned.shape[0]:
        chip, offset = divmod(first + done, part_rows)
        step = min(turned.shape[0] - done, part_rows - offset)
        out_ref[chip, base + offset : base + offset + step, :] = turned[done : done + step]
        done += step


def prepare_kernel(ids_ref, gates_ref, grads_ref, out_ref):
    ids = ids_ref[...].T
    gates = gates_ref[...].T
    chips, total, _ = out_ref.shape
    tokens, top = ids.shape
    width = grads_ref.shape[1]
    shape = (tokens, 256)
    lane = lax.broadcasted_iota(jnp.int32, shape, 1)
    rem = lane % 128
    expert = 16 * (rem // 8) + 8 * (lane // 128) + rem % 8
    hit = jnp.zeros(shape, F32)
    gate = jnp.zeros(shape, F32)
    for k in range(top):
        same = ids[:, k : k + 1] == expert
        hit = jnp.where(same, 1.0, hit)
        gate = jnp.where(same, gates[:, k : k + 1], gate)
    row = lax.broadcasted_iota(jnp.int32, (tokens, tokens), 0)
    col = lax.broadcasted_iota(jnp.int32, (tokens, tokens), 1)
    before = jnp.where(col < row, 1.0, 0.0).astype(BF16)
    pos = lax.dot_general(before, hit.astype(BF16), NN, preferred_element_type=F32)
    pos = jnp.where(hit > 0, pos, -1.0)
    token = lax.broadcasted_iota(jnp.int32, shape, 0).astype(F32)
    token_rows, gate_rows = [], []
    for c in range(CP):
        here = pos == c
        token_rows.append(jnp.max(jnp.where(here, token, -1.0), axis=0, keepdims=True))
        gate_rows.append(jnp.sum(jnp.where(here, gate, 0.0), axis=0, keepdims=True))
    table = jnp.concatenate(token_rows + gate_rows, axis=0).astype(BF16)
    table = jnp.concatenate([table[:, :128], table[:, 128:]], axis=0)
    codes_at = total - 4 * CP
    for j in range(chips):
        out_ref[j, codes_at:, :] = table
    copies = 4
    span = width // copies
    part = span // chips
    for p in range(copies):
        for n in range(span // 128):
            turned = grads_ref[:, p * span + n * 128 : p * span + (n + 1) * 128].T
            place_rows(out_ref, turned, n * 128, part, p * part)


def prepare(ids, gates, grads, chips):
    tokens, width = grads.shape
    return pl.pallas_call(
        prepare_kernel,
        out_shape=in_hbm((chips, width // chips + 4 * CP, tokens), BF16),
        compiler_params=params(),
        name="prepare",
    )(from_hbm(ids.T), from_hbm(gates.T), from_hbm(grads))


def turn_kernel(copy_ref, q_ref, out_ref):
    for n in range(q_ref.shape[1] // 128):
        out_ref[n * 128 : (n + 1) * 128, :] = q_ref[:, n * 128 : (n + 1) * 128].T


def turned_part(copy, q, copies):
    rows, width = q.shape
    steps = 2
    columns = width // copies
    return pl.pallas_call(
        turn_kernel,
        grid_spec=pltpu.PrefetchScalarGridSpec(
            num_scalar_prefetch=1,
            grid=(steps,),
            in_specs=[pl.BlockSpec((rows, columns // steps), lambda i, c: (0, c[0] * steps + i))],
            out_specs=pl.BlockSpec((columns // steps, rows), lambda i, c: (i, 0)),
        ),
        out_shape=in_hbm((columns, rows), BF16),
        compiler_params=params(),
        name="turned_part",
    )(copy, from_hbm(q))


def dispatch_kernel(core_ref, xt_ref, out_ref):
    core = core_ref[0]
    token = lax.broadcasted_iota(jnp.int32, (CP, 128), 1).astype(F32)
    group = 32
    width = out_ref.shape[2]
    start = pl.multiple_of(width + 2 * CP * core, 2 * CP)
    codes = []
    for i in range(2):
        table = xt_ref[i, pl.ds(start, 2 * CP), :].astype(F32)
        codes.append(table[:CP] + table[CP:])
    for g in range(128 // group):
        rows = []
        for i in range(2):
            parts = []
            for x in range(g * group, (g + 1) * group):
                u = codes[i][:, x : x + 1] - token
                parts.append(jnp.where((u > 0) & (u < 1), u, 0.0))
            picks = jnp.concatenate(parts, axis=0).astype(BF16)
            got = lax.dot_general(picks, xt_ref[i, :width], NT, preferred_element_type=F32)
            rows.append(got.reshape(group, CP, width))
        out_ref[g * group : (g + 1) * group] = jnp.concatenate(rows, axis=1).astype(BF16)


def dispatch(core, xt):
    chips, total, tokens = xt.shape
    width = total - 4 * CP

    def body(*refs):
        dispatch_kernel(*refs)

    return pl.pallas_call(
        body,
        grid_spec=pltpu.PrefetchScalarGridSpec(
            num_scalar_prefetch=1,
            grid=(chips // 2,),
            in_specs=[pl.BlockSpec((2, total, tokens), lambda i, _: (i, 0, 0))],
            out_specs=pl.BlockSpec((128, 2 * CP, width), lambda i, _: (0, i, 0)),
        ),
        out_shape=shape_of((128, chips * CP, width), BF16),
        compiler_params=params(),
        cost_estimate=pl.CostEstimate(
            flops=2 * 128 * CP * chips * tokens * width, bytes_accessed=128 * chips * CP * width * 2, transcendentals=0
        ),
    )(core, xt)


def arrived_rows(sources, rows_ref, sems, stream):
    step = pl.program_id(0)
    _, every, count, experts, _, _ = rows_ref.shape

    def copy(half, i):
        return pltpu.make_async_copy(
            sources[half].at[pl.ds(i * count, count), stream * experts : (stream + 1) * experts],
            rows_ref.at[half, i],
            sems.at[half, i],
        )

    @pl.when(step == 0)
    def _():
        for i in range(AHEAD):
            for half in range(2):
                copy(half, i).start()

    @pl.when(step + AHEAD < every)
    def _():
        for half in range(2):
            copy(half, step + AHEAD).start()

    for half in range(2):
        copy(half, step).wait()
    return rows_ref.at[0, step], rows_ref.at[1, step]


def mix_kernel(at_ref, own_ref, sib_ref, *rest, stream):
    q_refs, (out_ref, q_ref, tmp_ref, rows_ref, sems) = rest[:-5], rest[-5:]
    own_ref, sib_ref = arrived_rows((own_ref, sib_ref), rows_ref, sems, stream)
    core, copy = at_ref[0], at_ref[1]
    copies = len(q_refs)
    lanes = out_ref.shape[4]
    owner = lax.broadcasted_iota(jnp.int32, (128, lanes), 1) // 32
    for n in range(out_ref.shape[0]):
        part = q_refs[0].shape[1]
        for shift, ref in enumerate(q_refs):
            start = pl.multiple_of(part * ((copy + shift) % copies), 16)
            q_ref[pl.ds(start, part), :] = ref[n]
        for half, ref in enumerate((own_ref, sib_ref)):
            _, experts, rows, width = ref.shape
            got = lax.dot_general(
                ref[n].reshape(experts * rows, width), q_ref[...], NN, preferred_element_type=F32
            )
            acc = got[:rows]
            for x in range(1, experts):
                acc = jnp.where(owner == x, got[x * rows : (x + 1) * rows], acc)
            tmp_ref[...] = acc
            place = core if half == 0 else 1 - core
            for c in range(CAP):
                out_ref[n, c, place] = tmp_ref[pl.ds(c, 16, stride=CP), :].astype(BF16)


def mix(at, own, sib, q_parts, stream):
    chips, part, lanes = q_parts[0].shape
    lanes = lanes // STREAMS
    _, experts, rows, width = own.shape
    experts = experts // STREAMS
    step = STEP
    block = pl.BlockSpec(memory_space=pl.ANY)

    def body(*refs):
        mix_kernel(*refs, stream=stream)

    q_block = pl.BlockSpec((step, part, lanes), lambda i, _: (i, 0, stream))
    return pl.pallas_call(
        body,
        grid_spec=pltpu.PrefetchScalarGridSpec(
            num_scalar_prefetch=1,
            grid=(chips // step,),
            in_specs=[block, block] + [q_block] * len(q_parts),
            out_specs=pl.BlockSpec((step, CAP, 2, 16, lanes), lambda i, _: (i, 0, 0, 0, 0)),
            scratch_shapes=[
                pltpu.VMEM((width, lanes), BF16),
                pltpu.VMEM((rows, lanes), F32),
                pltpu.VMEM((2, chips // step, step, experts, rows, width), BF16),
                pltpu.SemaphoreType.DMA((2, chips // step)),
            ],
        ),
        out_shape=in_hbm((chips, CAP, 2, 16, lanes), BF16),
        compiler_params=params(),
        cost_estimate=pl.CostEstimate(
            flops=4 * chips * experts * rows * width * 256,
            bytes_accessed=4 * chips * experts * rows * width,
            transcendentals=0,
        ),
    )(at, own, sib, *q_parts)


def factor_kernel(copy_ref, parts_ref, hidden_ref, *refs):
    out_refs, (tmp_ref, lhs_ref) = refs[:-2], refs[-2:]
    copies = len(out_refs)
    step = pl.program_id(0)
    here = hidden_ref.shape[0]

    @pl.when(step == 0)
    def _():
        for c in range(CAP):
            for k in range(2):
                total = parts_ref[0, c, k].astype(F32)
                for j in range(1, parts_ref.shape[0]):
                    total = total + parts_ref[j, c, k].astype(F32)
                tmp_ref[pl.ds(k * CAP + c, 16, stride=2 * CAP), :] = total
        lhs_ref[...] = tmp_ref[...].T.astype(BF16)

    for n in range(here):
        start = pl.multiple_of((step * here + n) * 32, 32)
        lhs = lhs_ref[pl.ds(start, 32), 0 : hidden_ref.shape[1]]
        value = lax.dot_general(lhs, hidden_ref[n], NN, preferred_element_type=F32).astype(BF16)
        ahead = (step * here + n - copy_ref[0] + copies) % copies
        for k, out_ref in enumerate(out_refs):

            @pl.when(ahead == k)
            def _():
                out_ref[...] = value


def first_factor(copy, parts, hidden, stream, copies):
    experts, slots, units = hidden.shape
    experts = experts // STREAMS
    lanes = parts.shape[4]
    step = 2
    first = stream * experts // step
    return pl.pallas_call(
        factor_kernel,
        grid_spec=pltpu.PrefetchScalarGridSpec(
            num_scalar_prefetch=1,
            grid=(experts // step,),
            in_specs=[
                pl.BlockSpec(parts.shape, lambda i, _: (0, 0, 0, 0, 0)),
                pl.BlockSpec((step, slots, units), lambda i, _: (first + i, 0, 0)),
            ],
            out_specs=[pl.BlockSpec((32, units), lambda i, _: (0, 0))] * copies,
            scratch_shapes=[pltpu.VMEM((256, lanes), F32), pltpu.VMEM((lanes, 256), BF16)],
        ),
        out_shape=[shape_of((32, units), BF16)] * copies,
        compiler_params=params(),
        cost_estimate=pl.CostEstimate(
            flops=2 * experts * slots * units * 256, bytes_accessed=2 * experts * slots * units, transcendentals=0
        ),
    )(copy, parts, hidden)


def ortho_kernel(*refs):
    parts_refs, out_ref = refs[:-1], refs[-1]
    row = lax.broadcasted_iota(jnp.int32, (32, 32), 0)
    col = lax.broadcasted_iota(jnp.int32, (32, 32), 1)
    value = parts_refs[0][...].astype(F32)
    for ref in parts_refs[1:]:
        value = value + ref[...].astype(F32)
    gram = lax.dot_general(value, value, NT, precision=HIGHEST, preferred_element_type=F32)
    a = jnp.concatenate([gram, jnp.where(row == col, 1.0, 0.0)], axis=1)
    index = lax.broadcasted_iota(jnp.int32, (32, 64), 0)
    for k in range(32):
        inv = lax.rsqrt(a[k : k + 1, k : k + 1])
        pivot = a[k : k + 1, :] * inv
        lower = a[:, k : k + 1] * inv
        below = a - lower * pivot
        a = jnp.where(index > k, below, jnp.where(index == k, pivot, a))
    out_ref[...] = lax.dot_general(
        a[:, 32:], value, NN, precision=HIGHEST, preferred_element_type=F32
    ).astype(BF16)


def ortho_of(parts):
    rank, units = parts[0].shape
    return pl.pallas_call(
        ortho_kernel,
        out_shape=shape_of((rank, units), BF16),
        compiler_params=params(),
        cost_estimate=pl.CostEstimate(flops=5_000_000_000, bytes_accessed=4 * rank * units * 2, transcendentals=0),
    )(*parts)


def project_kernel(copy_ref, *refs, copies):
    part_refs, hidden_ref = refs[:copies], refs[copies]
    basis_ref, out_ref, ortho_ref, rows_ref = refs[-4:]
    step = pl.program_id(0)
    here, slots, units = hidden_ref.shape

    @pl.when(step == 0)
    def _():
        for k, ref in enumerate(part_refs):
            place = pl.multiple_of(32 * ((copy_ref[0] - k + copies) % copies), 32)
            ortho_ref[pl.ds(place, 32), :] = ref[...]

    start = pl.multiple_of(step * here * 32, 32)
    basis = ortho_ref[pl.ds(start, here * 32), :].astype(F32) * math.sqrt(units)
    basis_ref[...] = basis.reshape(here, 32, units)
    got = lax.dot_general(
        hidden_ref[...].reshape(here * slots, units), ortho_ref[...], NT, preferred_element_type=F32
    )
    owner = lax.broadcasted_iota(jnp.int32, (slots, ortho_ref.shape[0]), 1) // 32
    for n in range(here):
        value = got[n * slots : (n + 1) * slots]
        kept = rows_ref[...]
        rows_ref[...] = jnp.where(owner == step * here + n, value, kept)

    @pl.when(step == pl.num_programs(0) - 1)
    def _():
        for c in range(CAP):
            for k in range(2):
                value = rows_ref[pl.ds(k * CAP + c, 16, stride=2 * CAP), :].astype(BF16)
                for j in range(out_ref.shape[0]):
                    out_ref[j, c, k] = value


def project(copy, parts, hidden, stream, basis, chips):
    every, slots, units = hidden.shape
    experts = every // STREAMS
    copies = len(parts)
    lanes = experts * 32
    step = 2
    first = stream * experts // step
    given = [] if basis is None else [basis]

    def body(*refs):
        project_kernel(*refs, copies=copies)

    return pl.pallas_call(
        body,
        grid_spec=pltpu.PrefetchScalarGridSpec(
            num_scalar_prefetch=1,
            grid=(experts // step,),
            in_specs=[pl.BlockSpec((32, units), lambda i, _: (0, 0))] * copies
            + [pl.BlockSpec((step, slots, units), lambda i, _: (first + i, 0, 0))]
            + [pl.BlockSpec(memory_space=pl.ANY)] * len(given),
            out_specs=[
                pl.BlockSpec((step, 32, units), lambda i, _: (first + i, 0, 0)),
                pl.BlockSpec((chips, CAP, 2, 16, lanes), lambda i, _: (0, 0, 0, 0, 0)),
            ],
            scratch_shapes=[pltpu.VMEM((lanes, units), BF16), pltpu.VMEM((slots, lanes), F32)],
        ),
        out_shape=[
            shape_of((every, 32, units), F32),
            in_hbm((chips, CAP, 2, 16, lanes), BF16),
        ],
        input_output_aliases={copies + 2: 0} if given else {},
        compiler_params=params(),
        cost_estimate=pl.CostEstimate(
            flops=2 * experts * slots * units * 256, bytes_accessed=2 * experts * slots * units, transcendentals=0
        ),
    )(copy, *parts, hidden, *given)


def terms_kernel(at_ref, own_ref, sib_ref, proj_ref, *refs, stream):
    low_refs, high_refs, (rows_ref, sum_ref, held_ref, sems, sort_ref) = refs[:2], refs[2:4], refs[4:]
    core, copy = at_ref[0], at_ref[1]
    low = pl.program_id(0) < pl.num_programs(0) // 2

    def slot(p):
        apart = jnp.bitwise_xor(copy, p)
        mixed = jnp.where(low, jnp.where(apart == 1, 0, 3), jnp.where(apart == 1, 3, 0))
        return jnp.where(apart == 0, 2, jnp.where(apart == 2, 1, mixed))

    own_ref, sib_ref = arrived_rows((own_ref, sib_ref), held_ref, sems, stream)
    count, experts, _, width = own_ref.shape
    part = width // 4

    @pl.when(pl.program_id(0) == 0)
    def _():
        rows_ref[...] = jnp.zeros_like(rows_ref)
        sum_ref[...] = jnp.zeros_like(sum_ref)

    for n in range(count):
        for half in range(2):
            place = core if half == 0 else 1 - core
            for c in range(CAP):
                rows_ref[pl.ds(half * 128 + c, 16, stride=CP), :] = proj_ref[n, c, place].astype(F32)
        turned = rows_ref[...].T.astype(BF16)
        for x in range(experts):
            both = jnp.concatenate([own_ref[n, x], sib_ref[n, x]], axis=0)
            got = lax.dot_general(turned[x * 32 : (x + 1) * 32], both, NN, preferred_element_type=F32)
            sum_ref[x * 32 : (x + 1) * 32, 0:width] = got
        for i in range(4):
            tall = min(width - i * 128, 128)
            back = sum_ref[:, i * 128 : (i + 1) * 128].T[:tall].astype(BF16)
            done = 0
            while done < tall:
                p, offset = divmod(i * 128 + done, part)
                step = min(tall - done, part - offset)
                sort_ref[slot(p), n, offset : offset + step, :] = back[done : done + step]
                done += step
    for here, out_refs in ((low, low_refs), (jnp.logical_not(low), high_refs)):

        @pl.when(here)
        def _():
            out_refs[0][...] = sort_ref[0:2]
            out_refs[1][...] = sort_ref[2:4]


def second_terms(at, own, sib, proj, stream):
    chips, _, _, _, lanes = proj.shape
    _, experts, rows, width = own.shape
    experts = experts // STREAMS
    step = STEP
    half = chips // step // 2
    block = pl.BlockSpec(memory_space=pl.ANY)

    def body(*refs):
        terms_kernel(*refs, stream=stream)

    return pl.pallas_call(
        body,
        grid_spec=pltpu.PrefetchScalarGridSpec(
            num_scalar_prefetch=1,
            grid=(chips // step,),
            in_specs=[block, block, pl.BlockSpec((step, CAP, 2, 16, lanes), lambda i, _: (i, 0, 0, 0, 0))],
            out_specs=[
                pl.BlockSpec((2, step, width // 4, lanes), lambda i, _: (0, jnp.minimum(i, half - 1), 0, 0)),
                pl.BlockSpec((2, step, width // 4, lanes), lambda i, _: (0, jnp.minimum(i, half - 1), 0, 0)),
                pl.BlockSpec((2, step, width // 4, lanes), lambda i, _: (0, jnp.maximum(i - half, 0), 0, 0)),
                pl.BlockSpec((2, step, width // 4, lanes), lambda i, _: (0, jnp.maximum(i - half, 0), 0, 0)),
            ],
            scratch_shapes=[
                pltpu.VMEM((256, lanes), F32),
                pltpu.VMEM((lanes, 512), F32),
                pltpu.VMEM((2, chips // step, step, experts, rows, width), BF16),
                pltpu.SemaphoreType.DMA((2, chips // step)),
                pltpu.VMEM((4, step, width // 4, lanes), BF16),
            ],
        ),
        out_shape=[shape_of((2, chips // 2, width // 4, lanes), BF16)] * 4,
        compiler_params=params(),
        cost_estimate=pl.CostEstimate(
            flops=4 * chips * experts * rows * width * 256,
            bytes_accessed=4 * chips * experts * rows * width,
            transcendentals=0,
        ),
    )(at, own, sib, proj)


def gather_kernel(parts_ref, *refs):
    out_ref = refs[-1]
    total = parts_ref[0].astype(F32)
    for p in range(1, parts_ref.shape[0]):
        total = total + parts_ref[p].astype(F32)
    out_ref[...] = total.T


def owned_columns(parts, stream, sums):
    copies, columns, rows = parts.shape
    given = [] if sums is None else [sums]
    wide = 896
    return pl.pallas_call(
        gather_kernel,
        grid=(columns // wide,),
        in_specs=[pl.BlockSpec((copies, wide, rows), lambda i: (0, i, 0))]
        + [pl.BlockSpec(memory_space=pl.ANY)] * len(given),
        out_specs=pl.BlockSpec((rows, wide), lambda i: (stream, i)),
        out_shape=shape_of((rows * STREAMS, columns), F32),
        input_output_aliases={1: 0} if given else {},
        compiler_params=params(),
    )(parts, *given)


def exchange(values, axes):
    return lax.all_to_all(values, axes, split_axis=0, concat_axis=0, tiled=True)


def shift(value, step, copies):
    return lax.ppermute(value, "dp", [(i, (i + step) % copies) for i in range(copies)])


def first_sum_kernel(low_ref, low_got_ref, high_ref, high_got_ref, *out_refs):
    for k, (kept_ref, got_ref) in enumerate(((low_ref, low_got_ref), (high_ref, high_got_ref))):
        out_refs[2 * k][...] = kept_ref[0].astype(F32) + got_ref[0].astype(F32)
        out_refs[2 * k + 1][...] = (kept_ref[1].astype(F32) + got_ref[1].astype(F32)).astype(BF16)


def last_sum_kernel(low_ref, low_got_ref, high_ref, high_got_ref, out_ref):
    half = low_ref.shape[0]
    out_ref[:half] = (low_ref[...] + low_got_ref[...].astype(F32)).astype(BF16)
    out_ref[half:] = (high_ref[...] + high_got_ref[...].astype(F32)).astype(BF16)


def summed_over_copies(low_sent, low_kept, high_sent, high_kept, copies):
    near = [(i, i ^ 1) for i in range(copies)]
    far = [(i, i ^ 3) for i in range(copies)]
    _, chips, columns, lanes = low_kept.shape
    shape = (chips, columns, lanes)
    low_got = lax.ppermute(low_sent, "dp", near)
    high_got = lax.ppermute(high_sent, "dp", far)
    low, low_sent, high, high_sent = pl.pallas_call(
        first_sum_kernel, out_shape=[shape_of(shape, F32), shape_of(shape, BF16)] * 2, compiler_params=params()
    )(low_kept, low_got, high_kept, high_got)
    low_got = lax.ppermute(low_sent, "dp", far)
    high_got = lax.ppermute(high_sent, "dp", near)
    return pl.pallas_call(
        last_sum_kernel, out_shape=in_hbm((2 * chips, columns, lanes), BF16), compiler_params=params()
    )(low, low_got, high, high_got)


def around(part, copies):
    half = part.shape[0] // 2
    before = shift(part, 1, copies)
    after = shift(part, copies - 1, copies)
    far_low = shift(before[:half], 1, copies)
    far_high = shift(after[half:], copies - 1, copies)
    return [part, after, jnp.concatenate([far_low, far_high], axis=0), before]


def whole(out_grads, expert_ids, gate_probs, hidden_acts, q_previous):
    chips = lax.axis_size("chip")
    copies = lax.axis_size("dp")
    core = lax.axis_index("core").astype(jnp.int32).reshape(1)
    copy = lax.axis_index("dp").astype(jnp.int32).reshape(1)
    at = jnp.concatenate([core, copy])
    hidden = hidden_acts[0]
    experts, rank, width = q_previous.shape
    here = experts // STREAMS

    q_part = turned_part(copy, q_previous.reshape(experts * rank, width), copies)
    q_part = exchange(q_part.reshape(chips, -1, experts * rank), "chip")
    own_t = prepare(expert_ids[0], gate_probs[0], out_grads[0], chips)
    q_part, own_t = lax.optimization_barrier((q_part, own_t))
    q_parts = around(q_part, copies)
    own_t = exchange(own_t, "chip")
    sib_t = lax.ppermute(own_t, "core", [(0, 1), (1, 0)])
    own = dispatch(core, own_t)
    sib = dispatch(core, sib_t)
    own = own.reshape(chips, experts, *own.shape[1:])
    sib = sib.reshape(chips, experts, *sib.shape[1:])

    basis, sums = None, None
    for s in range(STREAMS):
        mixed = exchange(mix(at, own, sib, q_parts, s), "chip")
        factor = first_factor(copy, mixed, hidden, s, copies)
        factor = [factor[0]] + [shift(factor[k], k, copies) for k in range(1, copies)]
        ortho = ortho_of(factor)
        ortho = [ortho] + [shift(ortho, k, copies) for k in range(1, copies)]
        basis, proj = project(copy, ortho, hidden, s, basis, chips)
        proj = exchange(proj, "chip")
        terms = second_terms(at, own, sib, proj, s)
        terms = summed_over_copies(*terms, copies)
        terms = exchange(terms, "chip")
        sums = owned_columns(terms.reshape(1, width // copies, here * rank), s, sums)
    return (basis, sums.reshape(experts, rank, width // copies))


def solution(mesh):
    at = mesh.axis_names.index("expert")
    shape = mesh.devices.shape
    devices = mesh.devices.reshape(*shape[:at], shape[at] // 2, 2, *shape[at + 1 :])
    names = (*mesh.axis_names[:at], "chip", "core", *mesh.axis_names[at + 1 :])
    expert = ("chip", "core")
    return jax.shard_map(
        whole,
        mesh=Mesh(devices, names),
        in_specs=(
            P("dp", expert, None),
            P("dp", expert, None),
            P("dp", expert, None),
            P("dp", expert, None, None),
            P(expert, None, None),
        ),
        out_specs=(P(expert, None, None), P(expert, None, "dp")),
        check_vma=False,
    )
```

```python
import math

import jax
import jax.numpy as jnp
from jax import lax
from jax.experimental import pallas as pl
from jax.experimental.pallas import tpu as pltpu
from jax.sharding import Mesh, PartitionSpec as P


F32 = jnp.float32
BF16 = jnp.bfloat16
HIGHEST = lax.Precision.HIGHEST
NN = (((1,), (0,)), ((), ()))
NT = (((1,), (1,)), ((), ()))
CP = 8
CAP = 6
STREAMS = 2
BLOCKS = 4
GROUP = 32
MIX_STEP = 4
TERMS_STEP = 2
AHEAD = 3


def params(limit_mib=48, **kw):
    return pltpu.CompilerParams(vmem_limit_bytes=limit_mib * 2**20, **kw)


def shape_of(shape, dtype):
    return jax.ShapeDtypeStruct(shape, dtype)


def in_hbm(shape, dtype):
    return pltpu.HBM(shape, dtype)


def from_hbm(value):
    return pltpu.with_memory_space_constraint(value, pltpu.HBM)


def place_rows(out_ref, turned, first, part_rows, base):
    done = 0
    while done < turned.shape[0]:
        chip, offset = divmod(first + done, part_rows)
        step = min(turned.shape[0] - done, part_rows - offset)
        out_ref[chip, base + offset : base + offset + step, :] = turned[done : done + step]
        done += step


def prepare_kernel(ids_ref, gates_ref, grads_ref, out_ref):
    ids = ids_ref[...].T
    gates = gates_ref[...].T
    chips, total, _ = out_ref.shape
    tokens, top = ids.shape
    width = grads_ref.shape[1]
    shape = (tokens, 256)
    lane = lax.broadcasted_iota(jnp.int32, shape, 1)
    rem = lane % 128
    expert = 16 * (rem // 8) + 8 * (lane // 128) + rem % 8
    hit = jnp.zeros(shape, F32)
    gate = jnp.zeros(shape, F32)
    for k in range(top):
        same = ids[:, k : k + 1] == expert
        hit = jnp.where(same, 1.0, hit)
        gate = jnp.where(same, gates[:, k : k + 1], gate)
    row = lax.broadcasted_iota(jnp.int32, (tokens, tokens), 0)
    col = lax.broadcasted_iota(jnp.int32, (tokens, tokens), 1)
    before = jnp.where(col < row, 1.0, 0.0).astype(BF16)
    pos = lax.dot_general(before, hit.astype(BF16), NN, preferred_element_type=F32)
    pos = jnp.where(hit > 0, pos, -1.0)
    token = lax.broadcasted_iota(jnp.int32, shape, 0).astype(F32)
    token_rows, gate_rows = [], []
    for c in range(CP):
        here = pos == c
        token_rows.append(jnp.max(jnp.where(here, token, -1.0), axis=0, keepdims=True))
        gate_rows.append(jnp.sum(jnp.where(here, gate, 0.0), axis=0, keepdims=True))
    table = jnp.concatenate(token_rows + gate_rows, axis=0).astype(BF16)
    table = jnp.concatenate([table[:, :128], table[:, 128:]], axis=0)
    codes_at = total - 4 * CP
    for j in range(chips):
        out_ref[j, codes_at:, :] = table
    copies = 4
    span = width // copies
    part = span // chips
    for p in range(copies):
        for n in range(span // 128):
            turned = grads_ref[:, p * span + n * 128 : p * span + (n + 1) * 128].T
            place_rows(out_ref, turned, n * 128, part, p * part)


def prepare(ids, gates, grads, chips):
    tokens, width = grads.shape
    return pl.pallas_call(
        prepare_kernel,
        out_shape=in_hbm((chips, width // chips + 4 * CP, tokens), BF16),
        compiler_params=params(),
        name="prepare",
    )(from_hbm(ids.T), from_hbm(gates.T), from_hbm(grads))


def turn_kernel(copy_ref, q_ref, out_ref):
    for n in range(q_ref.shape[1] // 128):
        out_ref[n * 128 : (n + 1) * 128, :] = q_ref[:, n * 128 : (n + 1) * 128].T


def turned_part(copy, q, copies):
    rows, width = q.shape
    steps = 2
    columns = width // copies
    return pl.pallas_call(
        turn_kernel,
        grid_spec=pltpu.PrefetchScalarGridSpec(
            num_scalar_prefetch=1,
            grid=(steps,),
            in_specs=[pl.BlockSpec((rows, columns // steps), lambda i, c: (0, c[0] * steps + i))],
            out_specs=pl.BlockSpec((columns // steps, rows), lambda i, c: (i, 0)),
        ),
        out_shape=in_hbm((columns, rows), BF16),
        compiler_params=params(),
        name="turned_part",
    )(copy, from_hbm(q))


def dispatch_kernel(core_ref, xt_ref, out_ref):
    core = core_ref[0]
    token = lax.broadcasted_iota(jnp.int32, (CP, 128), 1).astype(F32)
    group = GROUP
    count = xt_ref.shape[0]
    width = out_ref.shape[2]
    start = pl.multiple_of(width + 2 * CP * core, 2 * CP)
    codes = []
    for i in range(count):
        table = xt_ref[i, pl.ds(start, 2 * CP), :].astype(F32)
        codes.append(table[:CP] + table[CP:])
    for g in range(128 // group):
        rows = []
        for i in range(count):
            parts = []
            for x in range(g * group, (g + 1) * group):
                u = codes[i][:, x : x + 1] - token
                parts.append(jnp.where((u > 0) & (u < 1), u, 0.0))
            picks = jnp.concatenate(parts, axis=0).astype(BF16)
            got = lax.dot_general(picks, xt_ref[i, :width], NT, preferred_element_type=F32)
            rows.append(got.reshape(group, CP, width))
        out_ref[g * group : (g + 1) * group] = jnp.concatenate(rows, axis=1).astype(BF16)


def dispatch(core, xt):
    chips, total, tokens = xt.shape
    width = total - 4 * CP

    def body(*refs):
        dispatch_kernel(*refs)

    return pl.pallas_call(
        body,
        grid_spec=pltpu.PrefetchScalarGridSpec(
            num_scalar_prefetch=1,
            grid=(chips // BLOCKS,),
            in_specs=[pl.BlockSpec((BLOCKS, total, tokens), lambda i, _: (i, 0, 0))],
            out_specs=pl.BlockSpec((128, BLOCKS * CP, width), lambda i, _: (0, i, 0)),
        ),
        out_shape=shape_of((128, chips * CP, width), BF16),
        compiler_params=params(),
        cost_estimate=pl.CostEstimate(
            flops=2 * 128 * CP * chips * tokens * width, bytes_accessed=128 * chips * CP * width * 2, transcendentals=0
        ),
    )(core, xt)


def arrived_rows(sources, rows_ref, sems, stream):
    step = pl.program_id(0)
    _, every, count, experts, _, _ = rows_ref.shape

    def copy(half, i):
        return pltpu.make_async_copy(
            sources[half].at[pl.ds(i * count, count), stream * experts : (stream + 1) * experts],
            rows_ref.at[half, i],
            sems.at[half, i],
        )

    @pl.when(step == 0)
    def _():
        for i in range(AHEAD):
            for half in range(2):
                copy(half, i).start()

    @pl.when(step + AHEAD < every)
    def _():
        for half in range(2):
            copy(half, step + AHEAD).start()

    for half in range(2):
        copy(half, step).wait()
    return rows_ref.at[0, step], rows_ref.at[1, step]


def mix_kernel(at_ref, own_ref, sib_ref, *rest, stream):
    q_refs, (out_ref, q_ref, tmp_ref, rows_ref, sems) = rest[:-5], rest[-5:]
    own_ref, sib_ref = arrived_rows((own_ref, sib_ref), rows_ref, sems, stream)
    core, copy = at_ref[0], at_ref[1]
    copies = len(q_refs)
    lanes = out_ref.shape[4]
    owner = lax.broadcasted_iota(jnp.int32, (128, lanes), 1) // 32
    for n in range(out_ref.shape[0]):
        part = q_refs[0].shape[1]
        for shift, ref in enumerate(q_refs):
            start = pl.multiple_of(part * ((copy + shift) % copies), 16)
            q_ref[pl.ds(start, part), :] = ref[n, :, stream * lanes : (stream + 1) * lanes]
        for half, ref in enumerate((own_ref, sib_ref)):
            _, experts, rows, width = ref.shape
            got = lax.dot_general(
                ref[n].reshape(experts * rows, width), q_ref[...], NN, preferred_element_type=F32
            )
            acc = got[:rows]
            for x in range(1, experts):
                acc = jnp.where(owner == x, got[x * rows : (x + 1) * rows], acc)
            tmp_ref[...] = acc
            place = core if half == 0 else 1 - core
            for c in range(CAP):
                out_ref[n, c, place] = tmp_ref[pl.ds(c, 16, stride=CP), :].astype(BF16)


def mix(at, own, sib, q_parts, stream):
    chips, part, lanes = q_parts[0].shape
    lanes = lanes // STREAMS
    _, experts, rows, width = own.shape
    experts = experts // STREAMS
    step = MIX_STEP
    block = pl.BlockSpec(memory_space=pl.ANY)

    def body(*refs):
        mix_kernel(*refs, stream=stream)

    q_block = pl.BlockSpec((step, part, lanes * STREAMS), lambda i, _: (i, 0, 0))
    return pl.pallas_call(
        body,
        grid_spec=pltpu.PrefetchScalarGridSpec(
            num_scalar_prefetch=1,
            grid=(chips // step,),
            in_specs=[block, block] + [q_block] * len(q_parts),
            out_specs=pl.BlockSpec((step, CAP, 2, 16, lanes), lambda i, _: (i, 0, 0, 0, 0)),
            scratch_shapes=[
                pltpu.VMEM((width, lanes), BF16),
                pltpu.VMEM((rows, lanes), F32),
                pltpu.VMEM((2, chips // step, step, experts, rows, width), BF16),
                pltpu.SemaphoreType.DMA((2, chips // step)),
            ],
        ),
        out_shape=in_hbm((chips, CAP, 2, 16, lanes), BF16),
        compiler_params=params(),
        cost_estimate=pl.CostEstimate(
            flops=4 * chips * experts * rows * width * 256,
            bytes_accessed=4 * chips * experts * rows * width,
            transcendentals=0,
        ),
    )(at, own, sib, *q_parts)


def factor_kernel(copy_ref, parts_ref, hidden_ref, *refs):
    out_refs, (tmp_ref, lhs_ref) = refs[:-2], refs[-2:]
    copies = len(out_refs)
    step = pl.program_id(0)
    here = hidden_ref.shape[0]

    @pl.when(step == 0)
    def _():
        for c in range(CAP):
            for k in range(2):
                total = parts_ref[0, c, k].astype(F32)
                for j in range(1, parts_ref.shape[0]):
                    total = total + parts_ref[j, c, k].astype(F32)
                tmp_ref[pl.ds(k * CAP + c, 16, stride=2 * CAP), :] = total
        lhs_ref[...] = tmp_ref[...].T.astype(BF16)

    for n in range(here):
        start = pl.multiple_of((step * here + n) * 32, 32)
        lhs = lhs_ref[pl.ds(start, 32), 0 : hidden_ref.shape[1]]
        value = lax.dot_general(lhs, hidden_ref[n], NN, preferred_element_type=F32).astype(BF16)
        ahead = (step * here + n - copy_ref[0] + copies) % copies
        for k, out_ref in enumerate(out_refs):

            @pl.when(ahead == k)
            def _():
                out_ref[...] = value


def first_factor(copy, parts, hidden, stream, copies):
    experts, slots, units = hidden.shape
    experts = experts // STREAMS
    lanes = parts.shape[4]
    step = 2
    first = stream * experts // step
    return pl.pallas_call(
        factor_kernel,
        grid_spec=pltpu.PrefetchScalarGridSpec(
            num_scalar_prefetch=1,
            grid=(experts // step,),
            in_specs=[
                pl.BlockSpec(parts.shape, lambda i, _: (0, 0, 0, 0, 0)),
                pl.BlockSpec((step, slots, units), lambda i, _: (first + i, 0, 0)),
            ],
            out_specs=[pl.BlockSpec((32, units), lambda i, _: (0, 0))] * copies,
            scratch_shapes=[pltpu.VMEM((256, lanes), F32), pltpu.VMEM((lanes, 256), BF16)],
        ),
        out_shape=[shape_of((32, units), BF16)] * copies,
        compiler_params=params(),
        cost_estimate=pl.CostEstimate(
            flops=2 * experts * slots * units * 256, bytes_accessed=2 * experts * slots * units, transcendentals=0
        ),
    )(copy, parts, hidden)


def ortho_kernel(*refs):
    parts_refs, out_ref = refs[:-1], refs[-1]
    row = lax.broadcasted_iota(jnp.int32, (32, 32), 0)
    col = lax.broadcasted_iota(jnp.int32, (32, 32), 1)
    value = parts_refs[0][...].astype(F32)
    for ref in parts_refs[1:]:
        value = value + ref[...].astype(F32)
    gram = lax.dot_general(value, value, NT, precision=HIGHEST, preferred_element_type=F32)
    a = jnp.concatenate([gram, jnp.where(row == col, 1.0, 0.0)], axis=1)
    index = lax.broadcasted_iota(jnp.int32, (32, 64), 0)
    for k in range(32):
        inv = lax.rsqrt(a[k : k + 1, k : k + 1])
        pivot = a[k : k + 1, :] * inv
        lower = a[:, k : k + 1] * inv
        below = a - lower * pivot
        a = jnp.where(index > k, below, jnp.where(index == k, pivot, a))
    out_ref[...] = lax.dot_general(
        a[:, 32:], value, NN, precision=HIGHEST, preferred_element_type=F32
    ).astype(BF16)


def ortho_of(parts):
    rank, units = parts[0].shape
    return pl.pallas_call(
        ortho_kernel,
        out_shape=shape_of((rank, units), BF16),
        compiler_params=params(),
        cost_estimate=pl.CostEstimate(flops=5_000_000_000, bytes_accessed=4 * rank * units * 2, transcendentals=0),
    )(*parts)


def project_kernel(copy_ref, *refs, copies):
    part_refs, hidden_ref = refs[:copies], refs[copies]
    basis_ref, out_ref, ortho_ref, rows_ref = refs[-4:]
    step = pl.program_id(0)
    here, slots, units = hidden_ref.shape

    @pl.when(step == 0)
    def _():
        for k, ref in enumerate(part_refs):
            place = pl.multiple_of(32 * ((copy_ref[0] - k + copies) % copies), 32)
            ortho_ref[pl.ds(place, 32), :] = ref[...]

    start = pl.multiple_of(step * here * 32, 32)
    basis = ortho_ref[pl.ds(start, here * 32), :].astype(F32) * math.sqrt(units)
    basis_ref[...] = basis.reshape(here, 32, units)
    got = lax.dot_general(
        hidden_ref[...].reshape(here * slots, units), ortho_ref[...], NT, preferred_element_type=F32
    )
    owner = lax.broadcasted_iota(jnp.int32, (slots, ortho_ref.shape[0]), 1) // 32
    for n in range(here):
        value = got[n * slots : (n + 1) * slots]
        kept = rows_ref[...]
        rows_ref[...] = jnp.where(owner == step * here + n, value, kept)

    @pl.when(step == pl.num_programs(0) - 1)
    def _():
        for c in range(CAP):
            for k in range(2):
                value = rows_ref[pl.ds(k * CAP + c, 16, stride=2 * CAP), :].astype(BF16)
                for j in range(out_ref.shape[0]):
                    out_ref[j, c, k] = value


def project(copy, parts, hidden, stream, basis, chips):
    every, slots, units = hidden.shape
    experts = every // STREAMS
    copies = len(parts)
    lanes = experts * 32
    step = 2
    first = stream * experts // step
    given = [] if basis is None else [basis]

    def body(*refs):
        project_kernel(*refs, copies=copies)

    return pl.pallas_call(
        body,
        grid_spec=pltpu.PrefetchScalarGridSpec(
            num_scalar_prefetch=1,
            grid=(experts // step,),
            in_specs=[pl.BlockSpec((32, units), lambda i, _: (0, 0))] * copies
            + [pl.BlockSpec((step, slots, units), lambda i, _: (first + i, 0, 0))]
            + [pl.BlockSpec(memory_space=pl.ANY)] * len(given),
            out_specs=[
                pl.BlockSpec((step, 32, units), lambda i, _: (first + i, 0, 0)),
                pl.BlockSpec((chips, CAP, 2, 16, lanes), lambda i, _: (0, 0, 0, 0, 0)),
            ],
            scratch_shapes=[pltpu.VMEM((lanes, units), BF16), pltpu.VMEM((slots, lanes), F32)],
        ),
        out_shape=[
            shape_of((every, 32, units), F32),
            in_hbm((chips, CAP, 2, 16, lanes), BF16),
        ],
        input_output_aliases={copies + 2: 0} if given else {},
        compiler_params=params(),
        cost_estimate=pl.CostEstimate(
            flops=2 * experts * slots * units * 256, bytes_accessed=2 * experts * slots * units, transcendentals=0
        ),
    )(copy, *parts, hidden, *given)


def terms_kernel(at_ref, own_ref, sib_ref, proj_ref, *refs, stream):
    low_refs, high_refs, (rows_ref, sum_ref, held_ref, sems, sort_ref) = refs[:2], refs[2:4], refs[4:]
    core, copy = at_ref[0], at_ref[1]
    low = pl.program_id(0) < pl.num_programs(0) // 2

    def slot(p):
        apart = jnp.bitwise_xor(copy, p)
        mixed = jnp.where(low, jnp.where(apart == 1, 0, 3), jnp.where(apart == 1, 3, 0))
        return jnp.where(apart == 0, 2, jnp.where(apart == 2, 1, mixed))

    own_ref, sib_ref = arrived_rows((own_ref, sib_ref), held_ref, sems, stream)
    count, experts, _, width = own_ref.shape
    part = width // 4

    @pl.when(pl.program_id(0) == 0)
    def _():
        rows_ref[...] = jnp.zeros_like(rows_ref)
        sum_ref[...] = jnp.zeros_like(sum_ref)

    for n in range(count):
        for half in range(2):
            place = core if half == 0 else 1 - core
            for c in range(CAP):
                rows_ref[pl.ds(half * 128 + c, 16, stride=CP), :] = proj_ref[n, c, place].astype(F32)
        turned = rows_ref[...].T.astype(BF16)
        for x in range(experts):
            both = jnp.concatenate([own_ref[n, x], sib_ref[n, x]], axis=0)
            got = lax.dot_general(turned[x * 32 : (x + 1) * 32], both, NN, preferred_element_type=F32)
            sum_ref[x * 32 : (x + 1) * 32, 0:width] = got
        for i in range(4):
            tall = min(width - i * 128, 128)
            back = sum_ref[:, i * 128 : (i + 1) * 128].T[:tall].astype(BF16)
            done = 0
            while done < tall:
                p, offset = divmod(i * 128 + done, part)
                step = min(tall - done, part - offset)
                sort_ref[slot(p), n, offset : offset + step, :] = back[done : done + step]
                done += step
    for here, out_refs in ((low, low_refs), (jnp.logical_not(low), high_refs)):

        @pl.when(here)
        def _():
            out_refs[0][...] = sort_ref[0:2]
            out_refs[1][...] = sort_ref[2:4]


def second_terms(at, own, sib, proj, stream):
    chips, _, _, _, lanes = proj.shape
    _, experts, rows, width = own.shape
    experts = experts // STREAMS
    step = TERMS_STEP
    half = chips // step // 2
    block = pl.BlockSpec(memory_space=pl.ANY)

    def body(*refs):
        terms_kernel(*refs, stream=stream)

    return pl.pallas_call(
        body,
        grid_spec=pltpu.PrefetchScalarGridSpec(
            num_scalar_prefetch=1,
            grid=(chips // step,),
            in_specs=[block, block, pl.BlockSpec((step, CAP, 2, 16, lanes), lambda i, _: (i, 0, 0, 0, 0))],
            out_specs=[
                pl.BlockSpec((2, step, width // 4, lanes), lambda i, _: (0, jnp.minimum(i, half - 1), 0, 0)),
                pl.BlockSpec((2, step, width // 4, lanes), lambda i, _: (0, jnp.minimum(i, half - 1), 0, 0)),
                pl.BlockSpec((2, step, width // 4, lanes), lambda i, _: (0, jnp.maximum(i - half, 0), 0, 0)),
                pl.BlockSpec((2, step, width // 4, lanes), lambda i, _: (0, jnp.maximum(i - half, 0), 0, 0)),
            ],
            scratch_shapes=[
                pltpu.VMEM((256, lanes), F32),
                pltpu.VMEM((lanes, 512), F32),
                pltpu.VMEM((2, chips // step, step, experts, rows, width), BF16),
                pltpu.SemaphoreType.DMA((2, chips // step)),
                pltpu.VMEM((4, step, width // 4, lanes), BF16),
            ],
        ),
        out_shape=[shape_of((2, chips // 2, width // 4, lanes), BF16)] * 4,
        compiler_params=params(),
        cost_estimate=pl.CostEstimate(
            flops=4 * chips * experts * rows * width * 256,
            bytes_accessed=4 * chips * experts * rows * width,
            transcendentals=0,
        ),
    )(at, own, sib, proj)


def gather_kernel(parts_ref, *refs):
    out_ref = refs[-1]
    total = parts_ref[0].astype(F32)
    for p in range(1, parts_ref.shape[0]):
        total = total + parts_ref[p].astype(F32)
    out_ref[...] = total.T


def owned_columns(parts, stream, sums):
    copies, columns, rows = parts.shape
    given = [] if sums is None else [sums]
    wide = 896
    return pl.pallas_call(
        gather_kernel,
        grid=(columns // wide,),
        in_specs=[pl.BlockSpec((copies, wide, rows), lambda i: (0, i, 0))]
        + [pl.BlockSpec(memory_space=pl.ANY)] * len(given),
        out_specs=pl.BlockSpec((rows, wide), lambda i: (stream, i)),
        out_shape=shape_of((rows * STREAMS, columns), F32),
        input_output_aliases={1: 0} if given else {},
        compiler_params=params(),
    )(parts, *given)


def exchange(values, axes):
    return lax.all_to_all(values, axes, split_axis=0, concat_axis=0, tiled=True)


def shift(value, step, copies):
    return lax.ppermute(value, "dp", [(i, (i + step) % copies) for i in range(copies)])


def first_sum_kernel(low_ref, low_got_ref, high_ref, high_got_ref, *out_refs):
    for k, (kept_ref, got_ref) in enumerate(((low_ref, low_got_ref), (high_ref, high_got_ref))):
        out_refs[2 * k][...] = kept_ref[0].astype(F32) + got_ref[0].astype(F32)
        out_refs[2 * k + 1][...] = (kept_ref[1].astype(F32) + got_ref[1].astype(F32)).astype(BF16)


def last_sum_kernel(low_ref, low_got_ref, high_ref, high_got_ref, out_ref):
    half = low_ref.shape[0]
    out_ref[:half] = (low_ref[...] + low_got_ref[...].astype(F32)).astype(BF16)
    out_ref[half:] = (high_ref[...] + high_got_ref[...].astype(F32)).astype(BF16)


def summed_over_copies(low_sent, low_kept, high_sent, high_kept, copies):
    near = [(i, i ^ 1) for i in range(copies)]
    far = [(i, i ^ 3) for i in range(copies)]
    _, chips, columns, lanes = low_kept.shape
    shape = (chips, columns, lanes)
    low_got = lax.ppermute(low_sent, "dp", near)
    high_got = lax.ppermute(high_sent, "dp", far)
    low, low_sent, high, high_sent = pl.pallas_call(
        first_sum_kernel, out_shape=[shape_of(shape, F32), shape_of(shape, BF16)] * 2, compiler_params=params()
    )(low_kept, low_got, high_kept, high_got)
    low_got = lax.ppermute(low_sent, "dp", far)
    high_got = lax.ppermute(high_sent, "dp", near)
    return pl.pallas_call(
        last_sum_kernel, out_shape=in_hbm((2 * chips, columns, lanes), BF16), compiler_params=params()
    )(low, low_got, high, high_got)


def around(part, copies):
    half = part.shape[0] // 2
    before = shift(part, 1, copies)
    after = shift(part, copies - 1, copies)
    far_low = shift(before[:half], 1, copies)
    far_high = shift(after[half:], copies - 1, copies)
    return [part, after, jnp.concatenate([far_low, far_high], axis=0), before]


def whole(out_grads, expert_ids, gate_probs, hidden_acts, q_previous):
    chips = lax.axis_size("chip")
    copies = lax.axis_size("dp")
    core = lax.axis_index("core").astype(jnp.int32).reshape(1)
    copy = lax.axis_index("dp").astype(jnp.int32).reshape(1)
    at = jnp.concatenate([core, copy])
    hidden = hidden_acts[0]
    experts, rank, width = q_previous.shape
    here = experts // STREAMS

    q_part = turned_part(copy, q_previous.reshape(experts * rank, width), copies)
    q_part = exchange(q_part.reshape(chips, -1, experts * rank), "chip")
    own_t = prepare(expert_ids[0], gate_probs[0], out_grads[0], chips)
    q_part, own_t = lax.optimization_barrier((q_part, own_t))
    q_parts = around(q_part, copies)
    own_t = exchange(own_t, "chip")
    sib_t = lax.ppermute(own_t, "core", [(0, 1), (1, 0)])
    own = dispatch(core, own_t)
    sib = dispatch(core, sib_t)
    own = own.reshape(chips, experts, *own.shape[1:])
    sib = sib.reshape(chips, experts, *sib.shape[1:])

    basis, sums = None, None
    for s in range(STREAMS):
        mixed = exchange(mix(at, own, sib, q_parts, s), "chip")
        factor = first_factor(copy, mixed, hidden, s, copies)
        factor = [factor[0]] + [shift(factor[k], k, copies) for k in range(1, copies)]
        ortho = ortho_of(factor)
        ortho = [ortho] + [shift(ortho, k, copies) for k in range(1, copies)]
        basis, proj = project(copy, ortho, hidden, s, basis, chips)
        proj = exchange(proj, "chip")
        terms = second_terms(at, own, sib, proj, s)
        terms = summed_over_copies(*terms, copies)
        terms = exchange(terms, "chip")
        sums = owned_columns(terms.reshape(1, width // copies, here * rank), s, sums)
    return (basis, sums.reshape(experts, rank, width // copies))


def solution(mesh):
    at = mesh.axis_names.index("expert")
    shape = mesh.devices.shape
    devices = mesh.devices.reshape(*shape[:at], shape[at] // 2, 2, *shape[at + 1 :])
    names = (*mesh.axis_names[:at], "chip", "core", *mesh.axis_names[at + 1 :])
    expert = ("chip", "core")
    return jax.shard_map(
        whole,
        mesh=Mesh(devices, names),
        in_specs=(
            P("dp", expert, None),
            P("dp", expert, None),
            P("dp", expert, None),
            P("dp", expert, None, None),
            P(expert, None, None),
        ),
        out_specs=(P(expert, None, None), P(expert, None, "dp")),
        check_vma=False,
    )
```

```python
import math

import jax
import jax.numpy as jnp
from jax import lax
from jax.experimental import pallas as pl
from jax.experimental.pallas import tpu as pltpu
from jax.sharding import Mesh, PartitionSpec as P


F32 = jnp.float32
BF16 = jnp.bfloat16
HIGHEST = lax.Precision.HIGHEST
NN = (((1,), (0,)), ((), ()))
NT = (((1,), (1,)), ((), ()))
CP = 8
CAP = 6
STREAMS = 2
BLOCKS = 4
GROUP = 32
MIX_STEP = 4
TERMS_STEP = 2
AHEAD = 3


def params(limit_mib=48, **kw):
    return pltpu.CompilerParams(vmem_limit_bytes=limit_mib * 2**20, **kw)


def shape_of(shape, dtype):
    return jax.ShapeDtypeStruct(shape, dtype)


def in_hbm(shape, dtype):
    return pltpu.HBM(shape, dtype)


def from_hbm(value):
    return pltpu.with_memory_space_constraint(value, pltpu.HBM)


def place_rows(out_ref, turned, first, part_rows, base):
    done = 0
    while done < turned.shape[0]:
        chip, offset = divmod(first + done, part_rows)
        step = min(turned.shape[0] - done, part_rows - offset)
        out_ref[chip, base + offset : base + offset + step, :] = turned[done : done + step]
        done += step


def prepare_kernel(ids_ref, gates_ref, grads_ref, out_ref):
    ids = ids_ref[...].T
    gates = gates_ref[...].T
    chips, total, _ = out_ref.shape
    tokens, top = ids.shape
    width = grads_ref.shape[1]
    shape = (tokens, 256)
    lane = lax.broadcasted_iota(jnp.int32, shape, 1)
    rem = lane % 128
    expert = 16 * (rem // 8) + 8 * (lane // 128) + rem % 8
    hit = jnp.zeros(shape, F32)
    gate = jnp.zeros(shape, F32)
    for k in range(top):
        same = ids[:, k : k + 1] == expert
        hit = jnp.where(same, 1.0, hit)
        gate = jnp.where(same, gates[:, k : k + 1], gate)
    row = lax.broadcasted_iota(jnp.int32, (tokens, tokens), 0)
    col = lax.broadcasted_iota(jnp.int32, (tokens, tokens), 1)
    before = jnp.where(col < row, 1.0, 0.0).astype(BF16)
    pos = lax.dot_general(before, hit.astype(BF16), NN, preferred_element_type=F32)
    pos = jnp.where(hit > 0, pos, -1.0)
    token = lax.broadcasted_iota(jnp.int32, shape, 0).astype(F32)
    token_rows, gate_rows = [], []
    for c in range(CP):
        here = pos == c
        token_rows.append(jnp.max(jnp.where(here, token, -1.0), axis=0, keepdims=True))
        gate_rows.append(jnp.sum(jnp.where(here, gate, 0.0), axis=0, keepdims=True))
    table = jnp.concatenate(token_rows + gate_rows, axis=0).astype(BF16)
    table = jnp.concatenate([table[:, :128], table[:, 128:]], axis=0)
    codes_at = total - 4 * CP
    for j in range(chips):
        out_ref[j, codes_at:, :] = table
    copies = 4
    span = width // copies
    part = span // chips
    for p in range(copies):
        for n in range(span // 128):
            turned = grads_ref[:, p * span + n * 128 : p * span + (n + 1) * 128].T
            place_rows(out_ref, turned, n * 128, part, p * part)


def prepare(ids, gates, grads, chips):
    tokens, width = grads.shape
    return pl.pallas_call(
        prepare_kernel,
        out_shape=in_hbm((chips, width // chips + 4 * CP, tokens), BF16),
        compiler_params=params(),
        name="prepare",
    )(from_hbm(ids.T), from_hbm(gates.T), from_hbm(grads))


def turn_kernel(copy_ref, q_ref, out_ref):
    for n in range(q_ref.shape[1] // 128):
        out_ref[n * 128 : (n + 1) * 128, :] = q_ref[:, n * 128 : (n + 1) * 128].T


def turned_part(copy, q, copies):
    rows, width = q.shape
    steps = 2
    columns = width // copies
    return pl.pallas_call(
        turn_kernel,
        grid_spec=pltpu.PrefetchScalarGridSpec(
            num_scalar_prefetch=1,
            grid=(steps,),
            in_specs=[pl.BlockSpec((rows, columns // steps), lambda i, c: (0, c[0] * steps + i))],
            out_specs=pl.BlockSpec((columns // steps, rows), lambda i, c: (i, 0)),
        ),
        out_shape=in_hbm((columns, rows), BF16),
        compiler_params=params(),
        name="turned_part",
    )(copy, from_hbm(q))


def dispatch_kernel(core_ref, xt_ref, out_ref):
    core = core_ref[0]
    token = lax.broadcasted_iota(jnp.int32, (CP, 128), 1).astype(F32)
    group = GROUP
    count = xt_ref.shape[0]
    width = out_ref.shape[2]
    start = pl.multiple_of(width + 2 * CP * core, 2 * CP)
    codes = []
    for i in range(count):
        table = xt_ref[i, pl.ds(start, 2 * CP), :].astype(F32)
        codes.append(table[:CP] + table[CP:])
    for g in range(128 // group):
        rows = []
        for i in range(count):
            parts = []
            for x in range(g * group, (g + 1) * group):
                u = codes[i][:, x : x + 1] - token
                parts.append(jnp.where((u > 0) & (u < 1), u, 0.0))
            picks = jnp.concatenate(parts, axis=0).astype(BF16)
            got = lax.dot_general(picks, xt_ref[i, :width], NT, preferred_element_type=F32)
            rows.append(got.reshape(group, CP, width))
        out_ref[g * group : (g + 1) * group] = jnp.concatenate(rows, axis=1).astype(BF16)


def dispatch(core, xt):
    chips, total, tokens = xt.shape
    width = total - 4 * CP

    def body(*refs):
        dispatch_kernel(*refs)

    return pl.pallas_call(
        body,
        grid_spec=pltpu.PrefetchScalarGridSpec(
            num_scalar_prefetch=1,
            grid=(chips // BLOCKS,),
            in_specs=[pl.BlockSpec((BLOCKS, total, tokens), lambda i, _: (i, 0, 0))],
            out_specs=pl.BlockSpec((128, BLOCKS * CP, width), lambda i, _: (0, i, 0)),
        ),
        out_shape=shape_of((128, chips * CP, width), BF16),
        compiler_params=params(),
        cost_estimate=pl.CostEstimate(
            flops=2 * 128 * CP * chips * tokens * width, bytes_accessed=128 * chips * CP * width * 2, transcendentals=0
        ),
    )(core, xt)


def arrived_rows(sources, rows_ref, sems, stream):
    step = pl.program_id(0)
    _, every, count, experts, _, _ = rows_ref.shape

    def copy(half, i):
        return pltpu.make_async_copy(
            sources[half].at[pl.ds(i * count, count), stream * experts : (stream + 1) * experts],
            rows_ref.at[half, i],
            sems.at[half, i],
        )

    @pl.when(step == 0)
    def _():
        for i in range(AHEAD):
            for half in range(2):
                copy(half, i).start()

    @pl.when(step + AHEAD < every)
    def _():
        for half in range(2):
            copy(half, step + AHEAD).start()

    for half in range(2):
        copy(half, step).wait()
    return rows_ref.at[0, step], rows_ref.at[1, step]


def mix_kernel(at_ref, own_ref, sib_ref, *rest, stream):
    q_refs, (out_ref, q_ref, tmp_ref, rows_ref, sems) = rest[:-5], rest[-5:]
    own_ref, sib_ref = arrived_rows((own_ref, sib_ref), rows_ref, sems, stream)
    core, copy = at_ref[0], at_ref[1]
    copies = 4
    lanes = out_ref.shape[4]
    low = pl.program_id(0) < pl.num_programs(0) // 2
    owner = lax.broadcasted_iota(jnp.int32, (128, lanes), 1) // 32
    for n in range(out_ref.shape[0]):
        part = q_refs[0].shape[1]
        here = slice(stream * lanes, (stream + 1) * lanes)
        for shift, ref in zip((0, 1, 3), q_refs):
            start = pl.multiple_of(part * ((copy + shift) % copies), 16)
            q_ref[pl.ds(start, part), :] = ref[n, :, here]
        start = pl.multiple_of(part * ((copy + 2) % copies), 16)
        q_ref[pl.ds(start, part), :] = jnp.where(low, q_refs[3][n, :, here], q_refs[4][n, :, here])
        for half, ref in enumerate((own_ref, sib_ref)):
            _, experts, rows, width = ref.shape
            got = lax.dot_general(
                ref[n].reshape(experts * rows, width), q_ref[...], NN, preferred_element_type=F32
            )
            acc = got[:rows]
            for x in range(1, experts):
                acc = jnp.where(owner == x, got[x * rows : (x + 1) * rows], acc)
            tmp_ref[...] = acc
            place = core if half == 0 else 1 - core
            for c in range(CAP):
                out_ref[n, c, place] = tmp_ref[pl.ds(c, 16, stride=CP), :].astype(BF16)


def mix(at, own, sib, q_parts, stream):
    chips, part, lanes = q_parts[0].shape
    lanes = lanes // STREAMS
    _, experts, rows, width = own.shape
    experts = experts // STREAMS
    step = MIX_STEP
    block = pl.BlockSpec(memory_space=pl.ANY)

    def body(*refs):
        mix_kernel(*refs, stream=stream)

    half = chips // step // 2
    q_shape = (step, part, lanes * STREAMS)
    q_blocks = [pl.BlockSpec(q_shape, lambda i, _: (i, 0, 0))] * 3 + [
        pl.BlockSpec(q_shape, lambda i, _: (jnp.minimum(i, half - 1), 0, 0)),
        pl.BlockSpec(q_shape, lambda i, _: (jnp.maximum(i - half, 0), 0, 0)),
    ]
    return pl.pallas_call(
        body,
        grid_spec=pltpu.PrefetchScalarGridSpec(
            num_scalar_prefetch=1,
            grid=(chips // step,),
            in_specs=[block, block] + q_blocks,
            out_specs=pl.BlockSpec((step, CAP, 2, 16, lanes), lambda i, _: (i, 0, 0, 0, 0)),
            scratch_shapes=[
                pltpu.VMEM((width, lanes), BF16),
                pltpu.VMEM((rows, lanes), F32),
                pltpu.VMEM((2, chips // step, step, experts, rows, width), BF16),
                pltpu.SemaphoreType.DMA((2, chips // step)),
            ],
        ),
        out_shape=in_hbm((chips, CAP, 2, 16, lanes), BF16),
        compiler_params=params(),
        cost_estimate=pl.CostEstimate(
            flops=4 * chips * experts * rows * width * 256,
            bytes_accessed=4 * chips * experts * rows * width,
            transcendentals=0,
        ),
    )(at, own, sib, *(from_hbm(q) for q in q_parts))


def factor_kernel(copy_ref, parts_ref, hidden_ref, *refs):
    out_refs, (tmp_ref, lhs_ref) = refs[:-2], refs[-2:]
    copies = len(out_refs)
    step = pl.program_id(0)
    here = hidden_ref.shape[0]

    @pl.when(step == 0)
    def _():
        for c in range(CAP):
            for k in range(2):
                total = parts_ref[0, c, k].astype(F32)
                for j in range(1, parts_ref.shape[0]):
                    total = total + parts_ref[j, c, k].astype(F32)
                tmp_ref[pl.ds(k * CAP + c, 16, stride=2 * CAP), :] = total
        lhs_ref[...] = tmp_ref[...].T.astype(BF16)

    for n in range(here):
        start = pl.multiple_of((step * here + n) * 32, 32)
        lhs = lhs_ref[pl.ds(start, 32), 0 : hidden_ref.shape[1]]
        value = lax.dot_general(lhs, hidden_ref[n], NN, preferred_element_type=F32).astype(BF16)
        ahead = (step * here + n - copy_ref[0] + copies) % copies
        for k, out_ref in enumerate(out_refs):

            @pl.when(ahead == k)
            def _():
                out_ref[...] = value


def first_factor(copy, parts, hidden, stream, copies):
    experts, slots, units = hidden.shape
    experts = experts // STREAMS
    lanes = parts.shape[4]
    step = 2
    first = stream * experts // step
    return pl.pallas_call(
        factor_kernel,
        grid_spec=pltpu.PrefetchScalarGridSpec(
            num_scalar_prefetch=1,
            grid=(experts // step,),
            in_specs=[
                pl.BlockSpec(parts.shape, lambda i, _: (0, 0, 0, 0, 0)),
                pl.BlockSpec((step, slots, units), lambda i, _: (first + i, 0, 0)),
            ],
            out_specs=[pl.BlockSpec((32, units), lambda i, _: (0, 0))] * copies,
            scratch_shapes=[pltpu.VMEM((256, lanes), F32), pltpu.VMEM((lanes, 256), BF16)],
        ),
        out_shape=[shape_of((32, units), BF16)] * copies,
        compiler_params=params(),
        cost_estimate=pl.CostEstimate(
            flops=2 * experts * slots * units * 256, bytes_accessed=2 * experts * slots * units, transcendentals=0
        ),
    )(copy, parts, hidden)


def ortho_kernel(*refs):
    parts_refs, out_ref = refs[:-1], refs[-1]
    row = lax.broadcasted_iota(jnp.int32, (32, 32), 0)
    col = lax.broadcasted_iota(jnp.int32, (32, 32), 1)
    value = parts_refs[0][...].astype(F32)
    for ref in parts_refs[1:]:
        value = value + ref[...].astype(F32)
    gram = lax.dot_general(value, value, NT, precision=HIGHEST, preferred_element_type=F32)
    a = jnp.concatenate([gram, jnp.where(row == col, 1.0, 0.0)], axis=1)
    index = lax.broadcasted_iota(jnp.int32, (32, 64), 0)
    for k in range(32):
        inv = lax.rsqrt(a[k : k + 1, k : k + 1])
        pivot = a[k : k + 1, :] * inv
        lower = a[:, k : k + 1] * inv
        below = a - lower * pivot
        a = jnp.where(index > k, below, jnp.where(index == k, pivot, a))
    out_ref[...] = lax.dot_general(
        a[:, 32:], value, NN, precision=HIGHEST, preferred_element_type=F32
    ).astype(BF16)


def ortho_of(parts):
    rank, units = parts[0].shape
    return pl.pallas_call(
        ortho_kernel,
        out_shape=shape_of((rank, units), BF16),
        compiler_params=params(),
        cost_estimate=pl.CostEstimate(flops=5_000_000_000, bytes_accessed=4 * rank * units * 2, transcendentals=0),
    )(*parts)


def project_kernel(copy_ref, *refs, copies):
    part_refs, hidden_ref = refs[:copies], refs[copies]
    basis_ref, out_ref, ortho_ref, rows_ref = refs[-4:]
    step = pl.program_id(0)
    here, slots, units = hidden_ref.shape

    @pl.when(step == 0)
    def _():
        for k, ref in enumerate(part_refs):
            place = pl.multiple_of(32 * ((copy_ref[0] - k + copies) % copies), 32)
            ortho_ref[pl.ds(place, 32), :] = ref[...]

    start = pl.multiple_of(step * here * 32, 32)
    basis = ortho_ref[pl.ds(start, here * 32), :].astype(F32) * math.sqrt(units)
    basis_ref[...] = basis.reshape(here, 32, units)
    got = lax.dot_general(
        hidden_ref[...].reshape(here * slots, units), ortho_ref[...], NT, preferred_element_type=F32
    )
    owner = lax.broadcasted_iota(jnp.int32, (slots, ortho_ref.shape[0]), 1) // 32
    for n in range(here):
        value = got[n * slots : (n + 1) * slots]
        kept = rows_ref[...]
        rows_ref[...] = jnp.where(owner == step * here + n, value, kept)

    @pl.when(step == pl.num_programs(0) - 1)
    def _():
        for c in range(CAP):
            for k in range(2):
                value = rows_ref[pl.ds(k * CAP + c, 16, stride=2 * CAP), :].astype(BF16)
                for j in range(out_ref.shape[0]):
                    out_ref[j, c, k] = value


def project(copy, parts, hidden, stream, basis, chips):
    every, slots, units = hidden.shape
    experts = every // STREAMS
    copies = len(parts)
    lanes = experts * 32
    step = 2
    first = stream * experts // step
    given = [] if basis is None else [basis]

    def body(*refs):
        project_kernel(*refs, copies=copies)

    return pl.pallas_call(
        body,
        grid_spec=pltpu.PrefetchScalarGridSpec(
            num_scalar_prefetch=1,
            grid=(experts // step,),
            in_specs=[pl.BlockSpec((32, units), lambda i, _: (0, 0))] * copies
            + [pl.BlockSpec((step, slots, units), lambda i, _: (first + i, 0, 0))]
            + [pl.BlockSpec(memory_space=pl.ANY)] * len(given),
            out_specs=[
                pl.BlockSpec((step, 32, units), lambda i, _: (first + i, 0, 0)),
                pl.BlockSpec((chips, CAP, 2, 16, lanes), lambda i, _: (0, 0, 0, 0, 0)),
            ],
            scratch_shapes=[pltpu.VMEM((lanes, units), BF16), pltpu.VMEM((slots, lanes), F32)],
        ),
        out_shape=[
            shape_of((every, 32, units), F32),
            in_hbm((chips, CAP, 2, 16, lanes), BF16),
        ],
        input_output_aliases={copies + 2: 0} if given else {},
        compiler_params=params(),
        cost_estimate=pl.CostEstimate(
            flops=2 * experts * slots * units * 256, bytes_accessed=2 * experts * slots * units, transcendentals=0
        ),
    )(copy, *parts, hidden, *given)


def terms_kernel(at_ref, own_ref, sib_ref, proj_ref, *refs, stream):
    low_refs, high_refs, (rows_ref, sum_ref, held_ref, sems, sort_ref) = refs[:2], refs[2:4], refs[4:]
    core, copy = at_ref[0], at_ref[1]
    low = pl.program_id(0) < pl.num_programs(0) // 2

    def slot(p):
        apart = jnp.bitwise_xor(copy, p)
        mixed = jnp.where(low, jnp.where(apart == 1, 0, 3), jnp.where(apart == 1, 3, 0))
        return jnp.where(apart == 0, 2, jnp.where(apart == 2, 1, mixed))

    own_ref, sib_ref = arrived_rows((own_ref, sib_ref), held_ref, sems, stream)
    count, experts, _, width = own_ref.shape
    part = width // 4

    @pl.when(pl.program_id(0) == 0)
    def _():
        rows_ref[...] = jnp.zeros_like(rows_ref)
        sum_ref[...] = jnp.zeros_like(sum_ref)

    for n in range(count):
        for half in range(2):
            place = core if half == 0 else 1 - core
            for c in range(CAP):
                rows_ref[pl.ds(half * 128 + c, 16, stride=CP), :] = proj_ref[n, c, place].astype(F32)
        turned = rows_ref[...].T.astype(BF16)
        for x in range(experts):
            both = jnp.concatenate([own_ref[n, x], sib_ref[n, x]], axis=0)
            got = lax.dot_general(turned[x * 32 : (x + 1) * 32], both, NN, preferred_element_type=F32)
            sum_ref[x * 32 : (x + 1) * 32, 0:width] = got
        for i in range(4):
            tall = min(width - i * 128, 128)
            back = sum_ref[:, i * 128 : (i + 1) * 128].T[:tall].astype(BF16)
            done = 0
            while done < tall:
                p, offset = divmod(i * 128 + done, part)
                step = min(tall - done, part - offset)
                sort_ref[slot(p), n, offset : offset + step, :] = back[done : done + step]
                done += step
    for here, out_refs in ((low, low_refs), (jnp.logical_not(low), high_refs)):

        @pl.when(here)
        def _():
            out_refs[0][...] = sort_ref[0:2]
            out_refs[1][...] = sort_ref[2:4]


def second_terms(at, own, sib, proj, stream):
    chips, _, _, _, lanes = proj.shape
    _, experts, rows, width = own.shape
    experts = experts // STREAMS
    step = TERMS_STEP
    half = chips // step // 2
    block = pl.BlockSpec(memory_space=pl.ANY)

    def body(*refs):
        terms_kernel(*refs, stream=stream)

    return pl.pallas_call(
        body,
        grid_spec=pltpu.PrefetchScalarGridSpec(
            num_scalar_prefetch=1,
            grid=(chips // step,),
            in_specs=[block, block, pl.BlockSpec((step, CAP, 2, 16, lanes), lambda i, _: (i, 0, 0, 0, 0))],
            out_specs=[
                pl.BlockSpec((2, step, width // 4, lanes), lambda i, _: (0, jnp.minimum(i, half - 1), 0, 0)),
                pl.BlockSpec((2, step, width // 4, lanes), lambda i, _: (0, jnp.minimum(i, half - 1), 0, 0)),
                pl.BlockSpec((2, step, width // 4, lanes), lambda i, _: (0, jnp.maximum(i - half, 0), 0, 0)),
                pl.BlockSpec((2, step, width // 4, lanes), lambda i, _: (0, jnp.maximum(i - half, 0), 0, 0)),
            ],
            scratch_shapes=[
                pltpu.VMEM((256, lanes), F32),
                pltpu.VMEM((lanes, 512), F32),
                pltpu.VMEM((2, chips // step, step, experts, rows, width), BF16),
                pltpu.SemaphoreType.DMA((2, chips // step)),
                pltpu.VMEM((4, step, width // 4, lanes), BF16),
            ],
        ),
        out_shape=[shape_of((2, chips // 2, width // 4, lanes), BF16)] * 4,
        compiler_params=params(),
        cost_estimate=pl.CostEstimate(
            flops=4 * chips * experts * rows * width * 256,
            bytes_accessed=4 * chips * experts * rows * width,
            transcendentals=0,
        ),
    )(at, own, sib, proj)


def gather_kernel(parts_ref, *refs):
    out_ref = refs[-1]
    total = parts_ref[0].astype(F32)
    for p in range(1, parts_ref.shape[0]):
        total = total + parts_ref[p].astype(F32)
    out_ref[...] = total.T


def owned_columns(parts, stream, sums):
    copies, columns, rows = parts.shape
    given = [] if sums is None else [sums]
    wide = 896
    return pl.pallas_call(
        gather_kernel,
        grid=(columns // wide,),
        in_specs=[pl.BlockSpec((copies, wide, rows), lambda i: (0, i, 0))]
        + [pl.BlockSpec(memory_space=pl.ANY)] * len(given),
        out_specs=pl.BlockSpec((rows, wide), lambda i: (stream, i)),
        out_shape=shape_of((rows * STREAMS, columns), F32),
        input_output_aliases={1: 0} if given else {},
        compiler_params=params(),
    )(parts, *given)


def exchange(values, axes):
    return lax.all_to_all(values, axes, split_axis=0, concat_axis=0, tiled=True)


def shift(value, step, copies):
    return lax.ppermute(value, "dp", [(i, (i + step) % copies) for i in range(copies)])


def first_sum_kernel(low_ref, low_got_ref, high_ref, high_got_ref, *out_refs):
    for k, (kept_ref, got_ref) in enumerate(((low_ref, low_got_ref), (high_ref, high_got_ref))):
        out_refs[2 * k][...] = kept_ref[0].astype(F32) + got_ref[0].astype(F32)
        out_refs[2 * k + 1][...] = (kept_ref[1].astype(F32) + got_ref[1].astype(F32)).astype(BF16)


def last_sum_kernel(low_ref, low_got_ref, high_ref, high_got_ref, out_ref):
    half = low_ref.shape[0]
    out_ref[:half] = (low_ref[...] + low_got_ref[...].astype(F32)).astype(BF16)
    out_ref[half:] = (high_ref[...] + high_got_ref[...].astype(F32)).astype(BF16)


def summed_over_copies(low_sent, low_kept, high_sent, high_kept, copies):
    near = [(i, i ^ 1) for i in range(copies)]
    far = [(i, i ^ 3) for i in range(copies)]
    _, chips, columns, lanes = low_kept.shape
    shape = (chips, columns, lanes)
    low_got = lax.ppermute(low_sent, "dp", near)
    high_got = lax.ppermute(high_sent, "dp", far)
    low, low_sent, high, high_sent = pl.pallas_call(
        first_sum_kernel, out_shape=[shape_of(shape, F32), shape_of(shape, BF16)] * 2, compiler_params=params()
    )(low_kept, low_got, high_kept, high_got)
    low_got = lax.ppermute(low_sent, "dp", far)
    high_got = lax.ppermute(high_sent, "dp", near)
    return pl.pallas_call(
        last_sum_kernel, out_shape=in_hbm((2 * chips, columns, lanes), BF16), compiler_params=params()
    )(low, low_got, high, high_got)


def around(part, copies):
    half = part.shape[0] // 2
    before = shift(part, 1, copies)
    after = shift(part, copies - 1, copies)
    far_low = shift(before[:half], 1, copies)
    far_high = shift(after[half:], copies - 1, copies)
    return [part, after, before, far_low, far_high]


def whole(out_grads, expert_ids, gate_probs, hidden_acts, q_previous):
    chips = lax.axis_size("chip")
    copies = lax.axis_size("dp")
    core = lax.axis_index("core").astype(jnp.int32).reshape(1)
    copy = lax.axis_index("dp").astype(jnp.int32).reshape(1)
    at = jnp.concatenate([core, copy])
    hidden = hidden_acts[0]
    experts, rank, width = q_previous.shape
    here = experts // STREAMS

    q_part = turned_part(copy, q_previous.reshape(experts * rank, width), copies)
    q_part = exchange(q_part.reshape(chips, -1, experts * rank), "chip")
    own_t = prepare(expert_ids[0], gate_probs[0], out_grads[0], chips)
    q_part, own_t = lax.optimization_barrier((q_part, own_t))
    q_parts = around(q_part, copies)
    own_t = exchange(own_t, "chip")
    sib_t = lax.ppermute(own_t, "core", [(0, 1), (1, 0)])
    own = dispatch(core, own_t)
    sib = dispatch(core, sib_t)
    own = own.reshape(chips, experts, *own.shape[1:])
    sib = sib.reshape(chips, experts, *sib.shape[1:])

    basis, sums = None, None
    for s in range(STREAMS):
        mixed = exchange(mix(at, own, sib, q_parts, s), "chip")
        factor = first_factor(copy, mixed, hidden, s, copies)
        factor = [factor[0]] + [shift(factor[k], k, copies) for k in range(1, copies)]
        ortho = ortho_of(factor)
        ortho = [ortho] + [shift(ortho, k, copies) for k in range(1, copies)]
        basis, proj = project(copy, ortho, hidden, s, basis, chips)
        proj = exchange(proj, "chip")
        terms = second_terms(at, own, sib, proj, s)
        terms = summed_over_copies(*terms, copies)
        terms = exchange(terms, "chip")
        sums = owned_columns(terms.reshape(1, width // copies, here * rank), s, sums)
    return (basis, sums.reshape(experts, rank, width // copies))


def solution(mesh):
    at = mesh.axis_names.index("expert")
    shape = mesh.devices.shape
    devices = mesh.devices.reshape(*shape[:at], shape[at] // 2, 2, *shape[at + 1 :])
    names = (*mesh.axis_names[:at], "chip", "core", *mesh.axis_names[at + 1 :])
    expert = ("chip", "core")
    return jax.shard_map(
        whole,
        mesh=Mesh(devices, names),
        in_specs=(
            P("dp", expert, None),
            P("dp", expert, None),
            P("dp", expert, None),
            P("dp", expert, None, None),
            P(expert, None, None),
        ),
        out_specs=(P(expert, None, None), P(expert, None, "dp")),
        check_vma=False,
    )
```

```python
import math

import jax
import jax.numpy as jnp
from jax import lax
from jax.experimental import pallas as pl
from jax.experimental.pallas import tpu as pltpu
from jax.sharding import Mesh, PartitionSpec as P


F32 = jnp.float32
BF16 = jnp.bfloat16
HIGHEST = lax.Precision.HIGHEST
NN = (((1,), (0,)), ((), ()))
NT = (((1,), (1,)), ((), ()))
CP = 8
CAP = 6
STREAMS = 2
BLOCKS = 4
GROUP = 32
MIX_STEP = 2
TERMS_STEP = 2
AHEAD = 3


def params(limit_mib=48, **kw):
    return pltpu.CompilerParams(vmem_limit_bytes=limit_mib * 2**20, **kw)


def shape_of(shape, dtype):
    return jax.ShapeDtypeStruct(shape, dtype)


def in_hbm(shape, dtype):
    return pltpu.HBM(shape, dtype)


def from_hbm(value):
    return pltpu.with_memory_space_constraint(value, pltpu.HBM)


def place_rows(out_ref, turned, first, part_rows, base):
    done = 0
    while done < turned.shape[0]:
        chip, offset = divmod(first + done, part_rows)
        step = min(turned.shape[0] - done, part_rows - offset)
        out_ref[chip, base + offset : base + offset + step, :] = turned[done : done + step]
        done += step


def prepare_kernel(ids_ref, gates_ref, grads_ref, out_ref):
    ids = ids_ref[...].T
    gates = gates_ref[...].T
    chips, total, _ = out_ref.shape
    tokens, top = ids.shape
    width = grads_ref.shape[1]
    shape = (tokens, 256)
    lane = lax.broadcasted_iota(jnp.int32, shape, 1)
    rem = lane % 128
    expert = 16 * (rem // 8) + 8 * (lane // 128) + rem % 8
    hit = jnp.zeros(shape, F32)
    gate = jnp.zeros(shape, F32)
    for k in range(top):
        same = ids[:, k : k + 1] == expert
        hit = jnp.where(same, 1.0, hit)
        gate = jnp.where(same, gates[:, k : k + 1], gate)
    row = lax.broadcasted_iota(jnp.int32, (tokens, tokens), 0)
    col = lax.broadcasted_iota(jnp.int32, (tokens, tokens), 1)
    before = jnp.where(col < row, 1.0, 0.0).astype(BF16)
    pos = lax.dot_general(before, hit.astype(BF16), NN, preferred_element_type=F32)
    pos = jnp.where(hit > 0, pos, -1.0)
    token = lax.broadcasted_iota(jnp.int32, shape, 0).astype(F32)
    token_rows, gate_rows = [], []
    for c in range(CP):
        here = pos == c
        token_rows.append(jnp.max(jnp.where(here, token, -1.0), axis=0, keepdims=True))
        gate_rows.append(jnp.sum(jnp.where(here, gate, 0.0), axis=0, keepdims=True))
    table = jnp.concatenate(token_rows + gate_rows, axis=0).astype(BF16)
    table = jnp.concatenate([table[:, :128], table[:, 128:]], axis=0)
    codes_at = total - 4 * CP
    for j in range(chips):
        out_ref[j, codes_at:, :] = table
    copies = 4
    span = width // copies
    part = span // chips
    for p in range(copies):
        for n in range(span // 128):
            turned = grads_ref[:, p * span + n * 128 : p * span + (n + 1) * 128].T
            place_rows(out_ref, turned, n * 128, part, p * part)


def prepare(ids, gates, grads, chips):
    tokens, width = grads.shape
    return pl.pallas_call(
        prepare_kernel,
        out_shape=in_hbm((chips, width // chips + 4 * CP, tokens), BF16),
        compiler_params=params(),
        name="prepare",
    )(from_hbm(ids.T), from_hbm(gates.T), from_hbm(grads))


def turn_kernel(copy_ref, q_ref, out_ref):
    for n in range(q_ref.shape[1] // 128):
        out_ref[n * 128 : (n + 1) * 128, :] = q_ref[:, n * 128 : (n + 1) * 128].T


def turned_part(copy, q, copies):
    rows, width = q.shape
    steps = 2
    columns = width // copies
    return pl.pallas_call(
        turn_kernel,
        grid_spec=pltpu.PrefetchScalarGridSpec(
            num_scalar_prefetch=1,
            grid=(steps,),
            in_specs=[pl.BlockSpec((rows, columns // steps), lambda i, c: (0, c[0] * steps + i))],
            out_specs=pl.BlockSpec((columns // steps, rows), lambda i, c: (i, 0)),
        ),
        out_shape=in_hbm((columns, rows), BF16),
        compiler_params=params(),
        name="turned_part",
    )(copy, from_hbm(q))


def dispatch_kernel(core_ref, xt_ref, out_ref):
    core = core_ref[0]
    token = lax.broadcasted_iota(jnp.int32, (CP, 128), 1).astype(F32)
    group = GROUP
    count = xt_ref.shape[0]
    width = out_ref.shape[2]
    start = pl.multiple_of(width + 2 * CP * core, 2 * CP)
    codes = []
    for i in range(count):
        table = xt_ref[i, pl.ds(start, 2 * CP), :].astype(F32)
        codes.append(table[:CP] + table[CP:])
    for g in range(128 // group):
        rows = []
        for i in range(count):
            parts = []
            for x in range(g * group, (g + 1) * group):
                u = codes[i][:, x : x + 1] - token
                parts.append(jnp.where((u > 0) & (u < 1), u, 0.0))
            picks = jnp.concatenate(parts, axis=0).astype(BF16)
            got = lax.dot_general(picks, xt_ref[i, :width], NT, preferred_element_type=F32)
            rows.append(got.reshape(group, CP, width))
        out_ref[g * group : (g + 1) * group] = jnp.concatenate(rows, axis=1).astype(BF16)


def dispatch(core, xt):
    chips, total, tokens = xt.shape
    width = total - 4 * CP

    def body(*refs):
        dispatch_kernel(*refs)

    return pl.pallas_call(
        body,
        grid_spec=pltpu.PrefetchScalarGridSpec(
            num_scalar_prefetch=1,
            grid=(chips // BLOCKS,),
            in_specs=[pl.BlockSpec((BLOCKS, total, tokens), lambda i, _: (i, 0, 0))],
            out_specs=pl.BlockSpec((128, BLOCKS * CP, width), lambda i, _: (0, i, 0)),
        ),
        out_shape=shape_of((128, chips * CP, width), BF16),
        compiler_params=params(),
        cost_estimate=pl.CostEstimate(
            flops=2 * 128 * CP * chips * tokens * width, bytes_accessed=128 * chips * CP * width * 2, transcendentals=0
        ),
    )(core, xt)


def arrived_rows(sources, rows_ref, sems, stream):
    step = pl.program_id(0)
    _, every, count, experts, _, _ = rows_ref.shape

    def copy(half, i):
        return pltpu.make_async_copy(
            sources[half].at[pl.ds(i * count, count), stream * experts : (stream + 1) * experts],
            rows_ref.at[half, i],
            sems.at[half, i],
        )

    @pl.when(step == 0)
    def _():
        for i in range(AHEAD):
            for half in range(2):
                copy(half, i).start()

    @pl.when(step + AHEAD < every)
    def _():
        for half in range(2):
            copy(half, step + AHEAD).start()

    for half in range(2):
        copy(half, step).wait()
    return rows_ref.at[0, step], rows_ref.at[1, step]


def mix_kernel(at_ref, own_ref, sib_ref, *rest, stream):
    q_refs, (out_ref, q_ref, tmp_ref, rows_ref, sems) = rest[:-5], rest[-5:]
    own_ref, sib_ref = arrived_rows((own_ref, sib_ref), rows_ref, sems, stream)
    core, copy = at_ref[0], at_ref[1]
    copies = len(q_refs)
    lanes = out_ref.shape[4]
    owner = lax.broadcasted_iota(jnp.int32, (128, lanes), 1) // 32
    for n in range(out_ref.shape[0]):
        part = q_refs[0].shape[1]
        for shift, ref in enumerate(q_refs):
            start = pl.multiple_of(part * ((copy + shift) % copies), 16)
            q_ref[pl.ds(start, part), :] = ref[n]
        for half, ref in enumerate((own_ref, sib_ref)):
            _, experts, rows, width = ref.shape
            got = lax.dot_general(
                ref[n].reshape(experts * rows, width), q_ref[...], NN, preferred_element_type=F32
            )
            acc = got[:rows]
            for x in range(1, experts):
                acc = jnp.where(owner == x, got[x * rows : (x + 1) * rows], acc)
            tmp_ref[...] = acc
            place = core if half == 0 else 1 - core
            for c in range(CAP):
                out_ref[n, c, place] = tmp_ref[pl.ds(c, 16, stride=CP), :].astype(BF16)


def mix(at, own, sib, q_parts, stream):
    chips, part, lanes = q_parts[0].shape
    lanes = lanes // STREAMS
    _, experts, rows, width = own.shape
    experts = experts // STREAMS
    step = MIX_STEP
    block = pl.BlockSpec(memory_space=pl.ANY)

    def body(*refs):
        mix_kernel(*refs, stream=stream)

    q_block = pl.BlockSpec((step, part, lanes), lambda i, _: (i, 0, stream))
    return pl.pallas_call(
        body,
        grid_spec=pltpu.PrefetchScalarGridSpec(
            num_scalar_prefetch=1,
            grid=(chips // step,),
            in_specs=[block, block] + [q_block] * len(q_parts),
            out_specs=pl.BlockSpec((step, CAP, 2, 16, lanes), lambda i, _: (i, 0, 0, 0, 0)),
            scratch_shapes=[
                pltpu.VMEM((width, lanes), BF16),
                pltpu.VMEM((rows, lanes), F32),
                pltpu.VMEM((2, chips // step, step, experts, rows, width), BF16),
                pltpu.SemaphoreType.DMA((2, chips // step)),
            ],
        ),
        out_shape=in_hbm((chips, CAP, 2, 16, lanes), BF16),
        compiler_params=params(),
        cost_estimate=pl.CostEstimate(
            flops=4 * chips * experts * rows * width * 256,
            bytes_accessed=4 * chips * experts * rows * width,
            transcendentals=0,
        ),
    )(at, own, sib, *(q if k == 2 else from_hbm(q) for k, q in enumerate(q_parts)))


def factor_kernel(copy_ref, parts_ref, hidden_ref, *refs):
    out_refs, (tmp_ref, lhs_ref) = refs[:-2], refs[-2:]
    copies = len(out_refs)
    step = pl.program_id(0)
    here = hidden_ref.shape[0]

    @pl.when(step == 0)
    def _():
        for c in range(CAP):
            for k in range(2):
                total = parts_ref[0, c, k].astype(F32)
                for j in range(1, parts_ref.shape[0]):
                    total = total + parts_ref[j, c, k].astype(F32)
                tmp_ref[pl.ds(k * CAP + c, 16, stride=2 * CAP), :] = total
        lhs_ref[...] = tmp_ref[...].T.astype(BF16)

    for n in range(here):
        start = pl.multiple_of((step * here + n) * 32, 32)
        lhs = lhs_ref[pl.ds(start, 32), 0 : hidden_ref.shape[1]]
        value = lax.dot_general(lhs, hidden_ref[n], NN, preferred_element_type=F32).astype(BF16)
        ahead = (step * here + n - copy_ref[0] + copies) % copies
        for k, out_ref in enumerate(out_refs):

            @pl.when(ahead == k)
            def _():
                out_ref[...] = value


def first_factor(copy, parts, hidden, stream, copies):
    experts, slots, units = hidden.shape
    experts = experts // STREAMS
    lanes = parts.shape[4]
    step = 2
    first = stream * experts // step
    return pl.pallas_call(
        factor_kernel,
        grid_spec=pltpu.PrefetchScalarGridSpec(
            num_scalar_prefetch=1,
            grid=(experts // step,),
            in_specs=[
                pl.BlockSpec(parts.shape, lambda i, _: (0, 0, 0, 0, 0)),
                pl.BlockSpec((step, slots, units), lambda i, _: (first + i, 0, 0)),
            ],
            out_specs=[pl.BlockSpec((32, units), lambda i, _: (0, 0))] * copies,
            scratch_shapes=[pltpu.VMEM((256, lanes), F32), pltpu.VMEM((lanes, 256), BF16)],
        ),
        out_shape=[shape_of((32, units), BF16)] * copies,
        compiler_params=params(),
        cost_estimate=pl.CostEstimate(
            flops=2 * experts * slots * units * 256, bytes_accessed=2 * experts * slots * units, transcendentals=0
        ),
    )(copy, parts, hidden)


def ortho_kernel(*refs):
    parts_refs, out_ref = refs[:-1], refs[-1]
    row = lax.broadcasted_iota(jnp.int32, (32, 32), 0)
    col = lax.broadcasted_iota(jnp.int32, (32, 32), 1)
    value = parts_refs[0][...].astype(F32)
    for ref in parts_refs[1:]:
        value = value + ref[...].astype(F32)
    gram = lax.dot_general(value, value, NT, precision=HIGHEST, preferred_element_type=F32)
    a = jnp.concatenate([gram, jnp.where(row == col, 1.0, 0.0)], axis=1)
    index = lax.broadcasted_iota(jnp.int32, (32, 64), 0)
    for k in range(32):
        inv = lax.rsqrt(a[k : k + 1, k : k + 1])
        pivot = a[k : k + 1, :] * inv
        lower = a[:, k : k + 1] * inv
        below = a - lower * pivot
        a = jnp.where(index > k, below, jnp.where(index == k, pivot, a))
    out_ref[...] = lax.dot_general(
        a[:, 32:], value, NN, precision=HIGHEST, preferred_element_type=F32
    ).astype(BF16)


def ortho_of(parts):
    rank, units = parts[0].shape
    return pl.pallas_call(
        ortho_kernel,
        out_shape=shape_of((rank, units), BF16),
        compiler_params=params(),
        cost_estimate=pl.CostEstimate(flops=5_000_000_000, bytes_accessed=4 * rank * units * 2, transcendentals=0),
    )(*parts)


def project_kernel(copy_ref, *refs, copies):
    part_refs, hidden_ref = refs[:copies], refs[copies]
    basis_ref, out_ref, ortho_ref, rows_ref = refs[-4:]
    step = pl.program_id(0)
    here, slots, units = hidden_ref.shape

    @pl.when(step == 0)
    def _():
        for k, ref in enumerate(part_refs):
            place = pl.multiple_of(32 * ((copy_ref[0] - k + copies) % copies), 32)
            ortho_ref[pl.ds(place, 32), :] = ref[...]

    start = pl.multiple_of(step * here * 32, 32)
    basis = ortho_ref[pl.ds(start, here * 32), :].astype(F32) * math.sqrt(units)
    basis_ref[...] = basis.reshape(here, 32, units)
    got = lax.dot_general(
        hidden_ref[...].reshape(here * slots, units), ortho_ref[...], NT, preferred_element_type=F32
    )
    owner = lax.broadcasted_iota(jnp.int32, (slots, ortho_ref.shape[0]), 1) // 32
    for n in range(here):
        value = got[n * slots : (n + 1) * slots]
        kept = rows_ref[...]
        rows_ref[...] = jnp.where(owner == step * here + n, value, kept)

    @pl.when(step == pl.num_programs(0) - 1)
    def _():
        for c in range(CAP):
            for k in range(2):
                value = rows_ref[pl.ds(k * CAP + c, 16, stride=2 * CAP), :].astype(BF16)
                for j in range(out_ref.shape[0]):
                    out_ref[j, c, k] = value


def project(copy, parts, hidden, stream, basis, chips):
    every, slots, units = hidden.shape
    experts = every // STREAMS
    copies = len(parts)
    lanes = experts * 32
    step = 2
    first = stream * experts // step
    given = [] if basis is None else [basis]

    def body(*refs):
        project_kernel(*refs, copies=copies)

    return pl.pallas_call(
        body,
        grid_spec=pltpu.PrefetchScalarGridSpec(
            num_scalar_prefetch=1,
            grid=(experts // step,),
            in_specs=[pl.BlockSpec((32, units), lambda i, _: (0, 0))] * copies
            + [pl.BlockSpec((step, slots, units), lambda i, _: (first + i, 0, 0))]
            + [pl.BlockSpec(memory_space=pl.ANY)] * len(given),
            out_specs=[
                pl.BlockSpec((step, 32, units), lambda i, _: (first + i, 0, 0)),
                pl.BlockSpec((chips, CAP, 2, 16, lanes), lambda i, _: (0, 0, 0, 0, 0)),
            ],
            scratch_shapes=[pltpu.VMEM((lanes, units), BF16), pltpu.VMEM((slots, lanes), F32)],
        ),
        out_shape=[
            shape_of((every, 32, units), F32),
            in_hbm((chips, CAP, 2, 16, lanes), BF16),
        ],
        input_output_aliases={copies + 2: 0} if given else {},
        compiler_params=params(),
        cost_estimate=pl.CostEstimate(
            flops=2 * experts * slots * units * 256, bytes_accessed=2 * experts * slots * units, transcendentals=0
        ),
    )(copy, *parts, hidden, *given)


def terms_kernel(at_ref, own_ref, sib_ref, proj_ref, *refs, stream):
    low_refs, high_refs, (rows_ref, sum_ref, held_ref, sems, sort_ref) = refs[:2], refs[2:4], refs[4:]
    core, copy = at_ref[0], at_ref[1]
    low = pl.program_id(0) < pl.num_programs(0) // 2

    def slot(p):
        apart = jnp.bitwise_xor(copy, p)
        mixed = jnp.where(low, jnp.where(apart == 1, 0, 3), jnp.where(apart == 1, 3, 0))
        return jnp.where(apart == 0, 2, jnp.where(apart == 2, 1, mixed))

    own_ref, sib_ref = arrived_rows((own_ref, sib_ref), held_ref, sems, stream)
    count, experts, _, width = own_ref.shape
    part = width // 4

    @pl.when(pl.program_id(0) == 0)
    def _():
        rows_ref[...] = jnp.zeros_like(rows_ref)
        sum_ref[...] = jnp.zeros_like(sum_ref)

    for n in range(count):
        for half in range(2):
            place = core if half == 0 else 1 - core
            for c in range(CAP):
                rows_ref[pl.ds(half * 128 + c, 16, stride=CP), :] = proj_ref[n, c, place].astype(F32)
        turned = rows_ref[...].T.astype(BF16)
        for x in range(experts):
            both = jnp.concatenate([own_ref[n, x], sib_ref[n, x]], axis=0)
            got = lax.dot_general(turned[x * 32 : (x + 1) * 32], both, NN, preferred_element_type=F32)
            sum_ref[x * 32 : (x + 1) * 32, 0:width] = got
        for i in range(4):
            tall = min(width - i * 128, 128)
            back = sum_ref[:, i * 128 : (i + 1) * 128].T[:tall].astype(BF16)
            done = 0
            while done < tall:
                p, offset = divmod(i * 128 + done, part)
                step = min(tall - done, part - offset)
                sort_ref[slot(p), n, offset : offset + step, :] = back[done : done + step]
                done += step
    for here, out_refs in ((low, low_refs), (jnp.logical_not(low), high_refs)):

        @pl.when(here)
        def _():
            out_refs[0][...] = sort_ref[0:2]
            out_refs[1][...] = sort_ref[2:4]


def second_terms(at, own, sib, proj, stream):
    chips, _, _, _, lanes = proj.shape
    _, experts, rows, width = own.shape
    experts = experts // STREAMS
    step = TERMS_STEP
    half = chips // step // 2
    block = pl.BlockSpec(memory_space=pl.ANY)

    def body(*refs):
        terms_kernel(*refs, stream=stream)

    return pl.pallas_call(
        body,
        grid_spec=pltpu.PrefetchScalarGridSpec(
            num_scalar_prefetch=1,
            grid=(chips // step,),
            in_specs=[block, block, pl.BlockSpec((step, CAP, 2, 16, lanes), lambda i, _: (i, 0, 0, 0, 0))],
            out_specs=[
                pl.BlockSpec((2, step, width // 4, lanes), lambda i, _: (0, jnp.minimum(i, half - 1), 0, 0)),
                pl.BlockSpec((2, step, width // 4, lanes), lambda i, _: (0, jnp.minimum(i, half - 1), 0, 0)),
                pl.BlockSpec((2, step, width // 4, lanes), lambda i, _: (0, jnp.maximum(i - half, 0), 0, 0)),
                pl.BlockSpec((2, step, width // 4, lanes), lambda i, _: (0, jnp.maximum(i - half, 0), 0, 0)),
            ],
            scratch_shapes=[
                pltpu.VMEM((256, lanes), F32),
                pltpu.VMEM((lanes, 512), F32),
                pltpu.VMEM((2, chips // step, step, experts, rows, width), BF16),
                pltpu.SemaphoreType.DMA((2, chips // step)),
                pltpu.VMEM((4, step, width // 4, lanes), BF16),
            ],
        ),
        out_shape=[shape_of((2, chips // 2, width // 4, lanes), BF16)] * 4,
        compiler_params=params(),
        cost_estimate=pl.CostEstimate(
            flops=4 * chips * experts * rows * width * 256,
            bytes_accessed=4 * chips * experts * rows * width,
            transcendentals=0,
        ),
    )(at, own, sib, proj)


def gather_kernel(parts_ref, *refs):
    out_ref = refs[-1]
    total = parts_ref[0].astype(F32)
    for p in range(1, parts_ref.shape[0]):
        total = total + parts_ref[p].astype(F32)
    out_ref[...] = total.T


def owned_columns(parts, stream, sums):
    copies, columns, rows = parts.shape
    given = [] if sums is None else [sums]
    wide = 896
    return pl.pallas_call(
        gather_kernel,
        grid=(columns // wide,),
        in_specs=[pl.BlockSpec((copies, wide, rows), lambda i: (0, i, 0))]
        + [pl.BlockSpec(memory_space=pl.ANY)] * len(given),
        out_specs=pl.BlockSpec((rows, wide), lambda i: (stream, i)),
        out_shape=shape_of((rows * STREAMS, columns), F32),
        input_output_aliases={1: 0} if given else {},
        compiler_params=params(),
    )(parts, *given)


def exchange(values, axes):
    return lax.all_to_all(values, axes, split_axis=0, concat_axis=0, tiled=True)


def shift(value, step, copies):
    return lax.ppermute(value, "dp", [(i, (i + step) % copies) for i in range(copies)])


def first_sum_kernel(low_ref, low_got_ref, high_ref, high_got_ref, *out_refs):
    for k, (kept_ref, got_ref) in enumerate(((low_ref, low_got_ref), (high_ref, high_got_ref))):
        out_refs[2 * k][...] = kept_ref[0].astype(F32) + got_ref[0].astype(F32)
        out_refs[2 * k + 1][...] = (kept_ref[1].astype(F32) + got_ref[1].astype(F32)).astype(BF16)


def last_sum_kernel(low_ref, low_got_ref, high_ref, high_got_ref, out_ref):
    half = low_ref.shape[0]
    out_ref[:half] = (low_ref[...] + low_got_ref[...].astype(F32)).astype(BF16)
    out_ref[half:] = (high_ref[...] + high_got_ref[...].astype(F32)).astype(BF16)


def summed_over_copies(low_sent, low_kept, high_sent, high_kept, copies):
    near = [(i, i ^ 1) for i in range(copies)]
    far = [(i, i ^ 3) for i in range(copies)]
    _, chips, columns, lanes = low_kept.shape
    shape = (chips, columns, lanes)
    low_got = lax.ppermute(low_sent, "dp", near)
    high_got = lax.ppermute(high_sent, "dp", far)
    low, low_sent, high, high_sent = pl.pallas_call(
        first_sum_kernel, out_shape=[shape_of(shape, F32), shape_of(shape, BF16)] * 2, compiler_params=params()
    )(low_kept, low_got, high_kept, high_got)
    low_got = lax.ppermute(low_sent, "dp", far)
    high_got = lax.ppermute(high_sent, "dp", near)
    return pl.pallas_call(
        last_sum_kernel, out_shape=in_hbm((2 * chips, columns, lanes), BF16), compiler_params=params()
    )(low, low_got, high, high_got)


def around(part, copies):
    half = part.shape[0] // 2
    before = shift(part, 1, copies)
    after = shift(part, copies - 1, copies)
    far_low = shift(before[:half], 1, copies)
    far_high = shift(after[half:], copies - 1, copies)
    return [part, after, jnp.concatenate([far_low, far_high], axis=0), before]


def whole(out_grads, expert_ids, gate_probs, hidden_acts, q_previous):
    chips = lax.axis_size("chip")
    copies = lax.axis_size("dp")
    core = lax.axis_index("core").astype(jnp.int32).reshape(1)
    copy = lax.axis_index("dp").astype(jnp.int32).reshape(1)
    at = jnp.concatenate([core, copy])
    hidden = hidden_acts[0]
    experts, rank, width = q_previous.shape
    here = experts // STREAMS

    q_part = turned_part(copy, q_previous.reshape(experts * rank, width), copies)
    q_part = exchange(q_part.reshape(chips, -1, experts * rank), "chip")
    own_t = prepare(expert_ids[0], gate_probs[0], out_grads[0], chips)
    q_part, own_t = lax.optimization_barrier((q_part, own_t))
    q_parts = around(q_part, copies)
    own_t = exchange(own_t, "chip")
    sib_t = lax.ppermute(own_t, "core", [(0, 1), (1, 0)])
    own = dispatch(core, own_t)
    sib = dispatch(core, sib_t)
    own = own.reshape(chips, experts, *own.shape[1:])
    sib = sib.reshape(chips, experts, *sib.shape[1:])

    basis, sums = None, None
    for s in range(STREAMS):
        mixed = exchange(mix(at, own, sib, q_parts, s), "chip")
        factor = first_factor(copy, mixed, hidden, s, copies)
        factor = [factor[0]] + [shift(factor[k], k, copies) for k in range(1, copies)]
        ortho = ortho_of(factor)
        ortho = [ortho] + [shift(ortho, k, copies) for k in range(1, copies)]
        basis, proj = project(copy, ortho, hidden, s, basis, chips)
        proj = exchange(proj, "chip")
        terms = second_terms(at, own, sib, proj, s)
        terms = summed_over_copies(*terms, copies)
        terms = exchange(terms, "chip")
        sums = owned_columns(terms.reshape(1, width // copies, here * rank), s, sums)
    return (basis, sums.reshape(experts, rank, width // copies))


def solution(mesh):
    at = mesh.axis_names.index("expert")
    shape = mesh.devices.shape
    devices = mesh.devices.reshape(*shape[:at], shape[at] // 2, 2, *shape[at + 1 :])
    names = (*mesh.axis_names[:at], "chip", "core", *mesh.axis_names[at + 1 :])
    expert = ("chip", "core")
    return jax.shard_map(
        whole,
        mesh=Mesh(devices, names),
        in_specs=(
            P("dp", expert, None),
            P("dp", expert, None),
            P("dp", expert, None),
            P("dp", expert, None, None),
            P(expert, None, None),
        ),
        out_specs=(P(expert, None, None), P(expert, None, "dp")),
        check_vma=False,
    )
```
